256 devices in a mesh: seq: 32 (over z, y), head: 8 (over x, core).
Axes of the slice: x: 4, y: 4, z: 8, core: 2. Of those that a mesh axis runs over, the one named last changes fastest.
Arguments:
- queries: bfloat16 [32768, 12288], P(('seq', 'head')), may hold values from -8 to 8
- latent: bfloat16 [32768, 512], P(('seq', 'head')), may hold values from -6 to 6
- rope_keys: bfloat16 [32768, 64], P(('seq', 'head')), may hold values from -8 to 8
- key_weight: bfloat16 [512, 8192], P('seq', 'head'), may hold values from -0.25 to 0.25
- value_weight: bfloat16 [512, 8192], P('seq', 'head'), may hold values from -0.25 to 0.25
- doc_lengths: int32 [128], replicated, may hold values from 1 to 510, as said below
Outputs:
- attended: bfloat16 [32768, 8192], P(('seq', 'head'))
The draws below stay inside these ranges and needn't reach their ends.
Inputs may be any that keep to these rules, and one draw needn't show every extreme that they name: `doc_lengths`: the documents lie in order in the pack and their lengths sum to 32768; document 0 starts at position 0 and every other document d starts strictly inside positions d * 256 to (d + 1) * 256 - 1, excluding the first of these; one length is exactly 510.
All inputs are finite; a program needn't handle non-finite values.
Results may differ from the reference program's by a relative error of at most 0.0062.
Values may be sent and summed in bfloat16 or wider, within the bound.
A program may use at most 64 MiB of HBM per device.

```python
import math
import jax
import jax.numpy as jnp
from jax import lax

KV_RANK = 512
NOPE = 128
ROPE = 64
VDIM = 128
HEADS = 64
TOK_DEV = 128
TOKENS = 32768
DOCS = 128
N_HEAD = 8


def draw_queries(key, part):
    shape = (TOKENS, HEADS, NOPE + ROPE)
    own_key = jax.random.fold_in(key, 11)
    drawn = jnp.clip(2.0 * jax.random.normal(own_key, shape, jnp.float32), -8.0, 8.0)
    return drawn.reshape(TOKENS, HEADS * (NOPE + ROPE)).astype(jnp.bfloat16)


def draw_rope_keys(key, part):
    shape = (TOKENS, ROPE)
    own_key = jax.random.fold_in(key, 12)
    drawn = jnp.clip(jax.random.normal(own_key, shape, jnp.float32), -8.0, 8.0)
    return drawn.astype(jnp.bfloat16)


def draw_doc_lengths(key, part):
    slot_rows = TOKENS // DOCS
    jitter = jax.random.randint(jax.random.fold_in(key, 21), (DOCS,), 1, slot_rows)
    chosen = jax.random.randint(jax.random.fold_in(key, 22), (), 1, DOCS - 1)
    index = jnp.arange(DOCS, dtype=jnp.int32)
    jitter = jnp.where(index == 1, jnp.minimum(jitter, slot_rows - 2), jitter)
    jitter = jnp.where(index == chosen, 1, jitter)
    jitter = jnp.where(index == chosen + 1, slot_rows - 1, jitter)
    jitter = jnp.where(index == 0, 0, jitter)
    starts = index * slot_rows + jitter
    ends = jnp.concatenate([starts[1:], jnp.full((1,), TOKENS, jnp.int32)])
    return (ends - starts).astype(jnp.int32)


def steps_of(key, dims, cuts, low, high):
    factor_of, own = 1.0, jax.random.fold_in(key, 6)
    for position, shards_of in cuts:
        heights = jnp.exp(jax.random.uniform(jax.random.fold_in(own, position), (shards_of,), jnp.float32, low / len(cuts), high / len(cuts)))
        factor_of = factor_of * jnp.repeat(heights, dims[position] // shards_of).reshape([-1 if axis == position else 1 for axis in range(len(dims))])
    return factor_of


def scatter_about(stream_key, extent, spread, bound, pieces=(), held_as=jnp.bfloat16):
    array = spread * jax.random.normal(stream_key, extent, jnp.float32)
    if pieces:
        array = array * steps_of(stream_key, extent, pieces, -0.22, 0.18)
    return jnp.clip(array, -bound, bound).astype(held_as)


def setup_inputs(seed: int = 0) -> dict:
    key_of = jax.random.split(jax.random.key(seed), 7)
    queries = draw_queries(jax.random.fold_in(key_of[6], 71), 0)
    latent = scatter_about(key_of[1], (TOKENS, KV_RANK), 1.0, 6.0, ((0, 256),))
    rope_keys = draw_rope_keys(jax.random.fold_in(key_of[6], 71), 0)
    key_weight = scatter_about(key_of[3], (KV_RANK, HEADS * NOPE), KV_RANK ** -0.5, 0.25, ((0, 32), (1, 8)))
    value_weight = scatter_about(key_of[4], (KV_RANK, HEADS * VDIM), KV_RANK ** -0.5, 0.25, ((0, 32), (1, 8)))
    doc_lengths = draw_doc_lengths(jax.random.fold_in(key_of[6], 71), 0)
    return dict(queries=queries, latent=latent, rope_keys=rope_keys, key_weight=key_weight, value_weight=value_weight, doc_lengths=doc_lengths)


def reference(queries, latent, rope_keys, key_weight, value_weight, doc_lengths):
    total_rows = queries.shape[0]
    group_rows = TOK_DEV * N_HEAD
    block_rows = min(512, group_rows)
    qk_width = NOPE + ROPE
    key_span = group_rows + block_rows
    score_scale = 1.0 / math.sqrt(qk_width)
    starts = (jnp.cumsum(doc_lengths) - doc_lengths).astype(jnp.int32)
    places = jnp.arange(total_rows, dtype=jnp.int32)
    started = (starts[None, :] <= places[:, None]).astype(jnp.int32)
    doc_of = (lax.optimization_barrier(jnp.sum(started, axis=1)) - 1).astype(jnp.int32)
    keys = jnp.dot(latent, key_weight, preferred_element_type=jnp.float32).astype(jnp.bfloat16)
    values = jnp.dot(latent, value_weight, preferred_element_type=jnp.float32).astype(jnp.bfloat16)
    keys_front = jnp.concatenate([jnp.zeros((group_rows, keys.shape[1]), jnp.bfloat16), keys], axis=0)
    values_front = jnp.concatenate([jnp.zeros((group_rows, values.shape[1]), jnp.bfloat16), values], axis=0)
    rope_front = jnp.concatenate([jnp.zeros((group_rows, ROPE), jnp.bfloat16), rope_keys], axis=0)
    docs_front = jnp.concatenate([-jnp.ones((group_rows,), jnp.int32), doc_of], axis=0)

    def one_block(q_index):
        q_start = (q_index * block_rows).astype(jnp.int32)
        q_block = lax.dynamic_slice_in_dim(queries, q_start, block_rows, 0).astype(jnp.float32)
        q_block = q_block.reshape(block_rows, HEADS, qk_width)
        k_nope = lax.dynamic_slice_in_dim(keys_front, q_start, key_span, 0).astype(jnp.float32)
        k_nope = k_nope.reshape(key_span, HEADS, NOPE)
        k_rope = lax.dynamic_slice_in_dim(rope_front, q_start, key_span, 0).astype(jnp.float32)
        k_values = lax.dynamic_slice_in_dim(values_front, q_start, key_span, 0).astype(jnp.float32)
        k_values = k_values.reshape(key_span, HEADS, VDIM)
        q_docs = lax.dynamic_slice_in_dim(doc_of, q_start, block_rows, 0)
        k_docs = lax.dynamic_slice_in_dim(docs_front, q_start, key_span, 0)
        q_places = q_start + jnp.arange(block_rows, dtype=jnp.int32)
        k_places = q_start - group_rows + jnp.arange(key_span, dtype=jnp.int32)
        scores = jnp.einsum('ihd,jhd->hij', q_block[:, :, :NOPE], k_nope)
        scores = (scores + jnp.einsum('ihd,jd->hij', q_block[:, :, NOPE:], k_rope)) * score_scale
        allowed = (q_docs[:, None] == k_docs[None, :]) & (k_places[None, :] <= q_places[:, None])
        scores = jnp.where(allowed[None, :, :], scores, -jnp.inf)
        row_peak = lax.optimization_barrier(jnp.max(scores, axis=2, keepdims=True))
        expo = jnp.exp(scores - row_peak)
        row_sum = lax.optimization_barrier(jnp.sum(expo, axis=2))
        rounded = lax.optimization_barrier(expo.astype(jnp.bfloat16)).astype(jnp.float32)
        mixed = jnp.einsum('hij,jhd->ihd', rounded, k_values) / jnp.transpose(row_sum)[:, :, None]
        return mixed.reshape(block_rows, HEADS * VDIM).astype(jnp.bfloat16)
    attended = lax.map(one_block, jnp.arange(total_rows // block_rows, dtype=jnp.int32))
    return attended.reshape(total_rows, HEADS * VDIM)
```

```python
import functools
import math

import jax
import jax.numpy as jnp
from jax import lax
from jax.experimental import pallas as pl
from jax.experimental.pallas import tpu as pltpu
from jax.sharding import PartitionSpec as P

NOPE = 128
ROPE = 64
VDIM = 128
QK = NOPE + ROPE
LOG2E = 1.4426950408889634
NY = 4

MESH = pl.DeviceIdType.MESH

FINE = (True, False, False, True)
RATE = 46.6e3
LATENCY = 2.3
HOP = 0.8
D2D_RATE = 300e3
BACKLOG = 1.5
SEND_COST = 0.04
WAIT_COST = 0.02
PIECE = (0.55, 0.45)


class Message:
    def __init__(self, name, deps, link, size, priority, units=None, where=None, move=None, hops=1):
        self.name, self.deps, self.link, self.size = name, deps, link, size
        self.priority, self.units, self.where, self.move, self.hops = priority, units, where, move, hops


def weight_messages(stages, nx, nz):
    tile = 16 * 128 * 2
    found = []

    def add(name, deps, axis, step, units, where, priority, blocks):
        move = {"x": 0, "z": 0, "y": 0}
        move[axis] = step
        hops = 2 if abs(step) == 2 else 1
        link = axis + ("+" if step > 0 else "-")
        found.append(
            Message(name, deps, link, blocks * units[1] * tile, priority, units, where, move, hops)
        )

    half = nz // 2
    for s in range(stages):
        for flow, (minor, last) in enumerate((("y", "x"), ("x", "y"))):
            both = (4 * s + 2 * flow, 2)
            first, second = (both[0], 1), (both[0] + 1, 1)

            def at(minor_at, last_at, z_at):
                return {minor: minor_at, last: last_at, "z": z_at}

            key = (s, flow)
            for k in (1, -1, 2):
                add((*key, "near", k), [], minor, k, both, at(0, 0, 0), (0, s), 1)
            near = [(*key, "near", k) for k in (1, -1, 2)]
            plus_far = s % 2 == 0
            reach = {1: half if plus_far else half - 1, -1: half - 1 if plus_far else half}
            came = {0: near}
            for way in (1, -1):
                for d in range(1, reach[way] + 1):
                    deps = near if d == 1 else [(*key, "z", way, d - 1)]
                    add((*key, "z", way, d), deps, "z", way, both, at(None, 0, -way * (d - 1)), (s, 0), 4)
                    came[-way * d] = [(*key, "z", way, d)]
            every = [name for names in came.values() for name in names]
            add((*key, "far"), near, last, 2, second, at(None, 0, 0), (s, 1), 4)
            for way in (1, -1):
                for d in range(1, reach[way] + 1):
                    deps = [(*key, "far")] if d == 1 else [(*key, "farz", way, d - 1)]
                    add((*key, "farz", way, d), deps, "z", way, second, at(None, 2, -way * (d - 1)), (s, 2), 4)
            if FINE[s]:
                for r, deps in came.items():
                    for way in (1, -1):
                        add((*key, "side", way, r), deps, last, way, both, at(None, 0, r), (s, 3), 4)
                    via = 1 if r in (0, -1, -2, -3) else -1
                    add(
                        (*key, "over", via, r), [(*key, "side", via, r)], last, via, first,
                        at(None, -via, r), (s, 2), 4,
                    )
            else:
                for way in (1, -1):
                    add((*key, "side", way), every, last, way, both, at(None, 0, None), (s, 3), 4 * nz)
                for way, part in ((1, (0, half)), (-1, (half, nz))):
                    add(
                        (*key, "over", way), [(*key, "side", way)], last, way, first,
                        at(None, -way, part), (s, 2), 4 * half,
                    )
    return found


def latent_messages(tok, rank):
    size = tok * (rank + 2 * ROPE) * 2
    return [
        Message(("next",), [], "x+", size, (0, 9), hops=1.5),
        Message(("mate",), [], "d2d", size, (0, 9)),
        Message(("share",), [("next",)], "d2d", size, (0, 9)),
    ]


def step_needs(messages, s, off):
    names = [m.name for m in messages if len(m.name) > 2]
    values = [n for n in names if n[0] == s and n[1] == 1]
    own = [n for n in names if n[0] == s and n[1] == 0 and n[2] in ("near", "z")]
    sides = {
        way: [n for n in names if n[0] == s and n[1] == 0 and n[2] == "side" and n[3] == way]
        for way in (1, -1)
    }
    opposite = [n for n in names if n[0] == s and n[1] == 0 and n[2] in ("over", "far", "farz")]
    return values + {0: own, -1: sides[1], 1: sides[-1], 2: opposite}[off]


OFFSETS = (0, -1, 1, 2)


def make_plan(messages, stages):
    by_name = {m.name: m for m in messages}
    pieces = [("setup", [("next",), ("mate",), ("share",)], 0.8)]
    for s in range(stages):
        for off in OFFSETS:
            for p, length in enumerate(PIECE):
                pieces.append(((s, off, p), step_needs(messages, s, off) if p == 0 else [], length))
    order, free, arrive, seen = [], {}, {}, set()
    waiting = sorted(messages, key=lambda m: m.priority)
    now, at_piece = 0.0, 0
    while waiting or arrive or at_piece < len(pieces):
        landed = sorted((t, str(n), n) for n, t in arrive.items() if t <= now)
        if landed:
            name = landed[0][2]
            del arrive[name]
            seen.add(name)
            order.append(("wait", name))
            now += WAIT_COST
            continue
        ready = [m for m in waiting if all(d in seen for d in m.deps)]
        able = [m for m in ready if free.get(m.link, 0.0) - now < BACKLOG]
        if able:
            m = able[0]
            waiting.remove(m)
            order.append(("send", m.name))
            now += SEND_COST
            rate = D2D_RATE if m.link == "d2d" else RATE
            begun = max(now, free.get(m.link, 0.0))
            free[m.link] = begun + m.size * max(1, m.hops) / rate
            arrive[m.name] = free[m.link] + LATENCY + HOP * (m.hops - 1)
            continue
        if at_piece < len(pieces) and all(n in seen for n in pieces[at_piece][1]):
            order.append(("piece", pieces[at_piece][0]))
            now += pieces[at_piece][2]
            at_piece += 1
            continue
        times = list(arrive.values()) + [free[m.link] - BACKLOG for m in ready]
        now = max(now, min(times)) + 1e-6
    return order, now


def kernel(
    sizes, queries, latent, key_weight, value_weight, lengths, out,
    w, lat, qbuf, kaug, rope_odd, vbuf, bias, obuf, len_buf,
    own_sem, lat_sem, len_sem, lat_send, w_recv, w_send, q_sem, q_send, o_sem, o_send, o_own,
):
    n_seq, n_head, stages = sizes
    nx, ny, nz = n_head // 2, NY, n_seq // NY
    tok, rank = latent.shape[0], latent.shape[1] - 2 * ROPE
    keys = 4 * tok
    seq, head = lax.axis_index("seq"), lax.axis_index("head")
    x, core = head // 2, head % 2
    z, y = seq // ny, seq % ny
    mate = 2 * x + 1 - core
    slot = seq * nx + x
    after, before = (slot + 1) % (n_seq * nx), (slot + n_seq * nx - 1) % (n_seq * nx)

    messages = weight_messages(stages, nx, nz) + latent_messages(tok, rank)
    order, _ = make_plan(messages, stages)
    by_name = {m.name: m for m in messages}
    number = {m.name: i for i, m in enumerate(messages)}

    def device(dx, dy, dz):
        return ((z + dz) % nz) * ny + (y + dy) % ny, ((x + dx) % nx) * 2 + core

    def chip(which):
        return which // nx, (which % nx) * 2 + core

    barrier = pltpu.get_barrier_semaphore()
    peers = [device(k, 0, 0) for k in range(1, nx)] + [device(0, k, 0) for k in range(1, ny)]
    peers += [device(0, 0, 1), device(0, 0, nz - 1), (seq, mate), chip(after), chip(before)]
    for peer in peers:
        pl.semaphore_signal(barrier, inc=1, device_id=peer, device_id_type=MESH)

    for s in range(stages):
        for kv, source in enumerate((key_weight, value_weight)):
            for j in range(2):
                pltpu.make_async_copy(
                    source.at[:, pl.ds((2 * s + j) * 128, 128)],
                    w.at[4 * s + 2 * kv + j, x, z, y], own_sem.at[s],
                ).start()
    pltpu.make_async_copy(latent, lat.at[2 + core], lat_sem.at[2 + core]).start()
    length_copy = pltpu.make_async_copy(lengths, len_buf, len_sem.at[0])
    length_copy.start()
    qw, cw = 2 * stages * QK, 2 * stages * VDIM

    def q_part(to_core, xi):
        return queries.at[:, pl.ds(pl.multiple_of((2 * xi + to_core) * qw, 128), qw)]

    for xi in range(nx):
        pltpu.make_async_copy(q_part(core, xi), qbuf.at[core, xi], q_sem.at[core, xi]).start()

    for s in range(stages):
        landed = w.at[pl.ds(4 * s, 4), x, z, y]
        pltpu.make_async_copy(landed, landed, own_sem.at[s]).wait()
    pl.semaphore_wait(barrier, len(peers))

    def place(at, here, n):
        if at is None:
            return pl.ds(0, n)
        if isinstance(at, tuple):
            return pl.ds(at[0], at[1] - at[0])
        return (here + at % n) % n

    def block(m, sent):
        back = {a: 0 if sent else m.move[a] for a in "xyz"}

        def shifted(a):
            at = m.where[a]
            return at - back[a] if isinstance(at, int) else at

        return w.at[
            pl.ds(*m.units), place(shifted("x"), x, nx), place(shifted("z"), z, nz), place(shifted("y"), y, ny)
        ]

    def copy_of(name):
        m = by_name[name]
        if name == ("next",):
            return pltpu.make_async_remote_copy(
                src_ref=latent, dst_ref=lat.at[core], send_sem=lat_send.at[0],
                recv_sem=lat_sem.at[core], device_id=chip(after), device_id_type=MESH,
            )
        if name == ("mate",):
            return pltpu.make_async_remote_copy(
                src_ref=latent, dst_ref=lat.at[2 + core], send_sem=lat_send.at[1],
                recv_sem=lat_sem.at[2 + core], device_id=(seq, mate), device_id_type=MESH,
            )
        if name == ("share",):
            return pltpu.make_async_remote_copy(
                src_ref=lat.at[core], dst_ref=lat.at[core], send_sem=lat_send.at[2],
                recv_sem=lat_sem.at[core], device_id=(seq, mate), device_id_type=MESH,
            )
        sent = block(m, True)
        i = number[name]
        return pltpu.make_async_remote_copy(
            src_ref=sent, dst_ref=sent, send_sem=w_send.at[i], recv_sem=w_recv.at[i],
            device_id=device(m.move["x"], m.move["y"], m.move["z"]), device_id_type=MESH,
        )

    def lat_wait(at):
        pltpu.make_async_copy(lat.at[at], lat.at[at], lat_sem.at[at]).wait()

    def take(name):
        if name == ("next",):
            lat_wait(core)
        elif name == ("mate",):
            lat_wait(3 - core)
        elif name == ("share",):
            lat_wait(1 - core)
        else:
            landed = block(by_name[name], False)
            pltpu.make_async_copy(landed, landed, w_recv.at[number[name]]).wait()

    def q_copy(xi):
        return pltpu.make_async_remote_copy(
            src_ref=q_part(1 - core, xi), dst_ref=qbuf.at[core, xi], send_sem=q_send.at[xi],
            recv_sem=q_sem.at[core, xi], device_id=(seq, mate), device_id_type=MESH,
        )

    def setup():
        lat_wait(2 + core)
        length_copy.wait()
        lane = lax.broadcasted_iota(jnp.int32, (1, lengths.shape[1]), 1)
        start_own = jnp.sum(jnp.where(lane < slot, len_buf[...], 0), axis=1, keepdims=True)
        start_last = jnp.sum(jnp.where(lane < slot - 1, len_buf[...], 0), axis=1, keepdims=True)
        first = slot * 2 * tok
        q_place = first + lax.broadcasted_iota(jnp.int32, (2 * tok, 1), 0)
        begun = jnp.where(q_place >= start_own, start_own, start_last)
        k_place = first - 2 * tok + lax.broadcasted_iota(jnp.int32, (2 * tok, keys), 1)
        bias[...] = jnp.where((k_place >= begun) & (k_place <= q_place), 0.0, -jnp.inf)
        tail = lat[:, :, rank:].reshape(keys, 2 * ROPE)
        kaug[0, :, NOPE:] = tail
        rope_odd[...] = pltpu.roll(tail.astype(jnp.float32), ROPE, axis=1)
        for xi in range(nx):
            for t in range(2):
                pltpu.make_async_copy(qbuf.at[t, xi], qbuf.at[t, xi], q_sem.at[t, xi]).wait()

    scale = LOG2E / math.sqrt(QK)

    def weights(s, j, xi):
        parts = [w[4 * s + j + i, xi].reshape(n_seq * 16, 128) for i in range(2)]
        return jnp.concatenate(parts, axis=1)

    def project(s, xi):
        tokens = lat[:, :, :rank].reshape(keys, rank)
        low = lax.broadcasted_iota(jnp.int32, (keys, NOPE), 1) < ROPE
        k = jnp.dot(tokens, weights(s, 0, xi), preferred_element_type=jnp.float32)
        kaug[0, :, :NOPE] = k[:, :NOPE].astype(jnp.bfloat16)
        turned = pltpu.roll(k[:, NOPE:], ROPE, axis=1)
        kaug[1, :, :NOPE] = jnp.where(low, 0.0, turned).astype(jnp.bfloat16)
        kaug[1, :, NOPE:] = jnp.where(low, turned, rope_odd[...]).astype(jnp.bfloat16)
        v = jnp.dot(tokens, weights(s, 2, xi), preferred_element_type=jnp.float32)
        vbuf[...] = v.astype(jnp.bfloat16)

    def attend(s, xi):
        for t in range(2):
            span = (3 + t) * tok
            hide = bias[t * tok:(t + 1) * tok, :span]
            for h in range(2):
                begin = pl.multiple_of(s * 2 * QK + h * NOPE, 128)
                q = qbuf[t, xi, :, pl.ds(begin, 2 * NOPE)]
                sc = lax.dot_general(
                    q, kaug[h, :span, :], (((1,), (1,)), ((), ())),
                    preferred_element_type=jnp.float32,
                )
                sc = sc * scale + hide
                peak = jnp.max(sc, axis=1, keepdims=True)
                expo = jnp.exp2(sc - peak)
                total = jnp.sum(expo, axis=1, keepdims=True)
                cols = slice(h * VDIM, (h + 1) * VDIM)
                mixed = jnp.dot(
                    expo.astype(jnp.bfloat16), vbuf[:span, cols],
                    preferred_element_type=jnp.float32,
                )
                obuf[t, s, xi, :, cols] = (mixed / total).astype(jnp.bfloat16)

    def out_part(s, xi):
        at = pl.multiple_of((2 * xi + core) * cw + s * 2 * VDIM, 128)
        return out.at[:, pl.ds(at, 2 * VDIM)]

    def give_own(s, xi):
        return pltpu.make_async_copy(obuf.at[core, s, xi], out_part(s, xi), o_own.at[s, xi])

    def give_mate(s, xi):
        return pltpu.make_async_remote_copy(
            src_ref=obuf.at[1 - core, s, xi], dst_ref=out_part(s, xi), send_sem=o_send.at[s, xi],
            recv_sem=o_sem.at[s, xi], device_id=(seq, mate), device_id_type=MESH,
        )

    def act(kind, name):
        if kind == "send":
            copy_of(name).start()
        else:
            take(name)

    prologue, slots, current = [], {}, None
    for kind, name in order:
        if kind == "piece" and name != "setup":
            s, off, p = name
            current = (s * nx + OFFSETS.index(off), p)
            slots[current] = []
        elif current is None:
            prologue.append((kind, name))
        else:
            slots[current].append((kind, name))

    for kind, name in prologue:
        if kind == "piece":
            for xi in range(nx):
                q_copy(xi).start()
            setup()
        else:
            act(kind, name)

    def step(i, carry):
        s, turn = i // nx, i % nx
        off = jnp.where(turn == 0, 0, jnp.where(turn == 1, nx - 1, jnp.where(turn == 2, 1, 2)))
        xi = (x + off) % nx

        def events(p, low, high):
            if not any(slots[(k, p)] for k in range(low, high)):
                return
            if high - low == 1:
                for kind, name in slots[(low, p)]:
                    act(kind, name)
                return
            middle = (low + high) // 2
            pl.when(i < middle)(functools.partial(events, p, low, middle))
            pl.when(i >= middle)(functools.partial(events, p, middle, high))

        project(s, xi)
        events(0, 0, stages * nx)
        attend(s, xi)
        give_own(s, xi).start()
        give_mate(s, xi).start()
        events(1, 0, stages * nx)
        return carry

    lax.fori_loop(0, stages * nx, step, 0)

    def close(i, carry):
        s, xi = i // nx, i % nx
        give_own(s, xi).wait()
        give_mate(s, xi).wait_send()
        landed = out_part(s, xi)
        at = pl.multiple_of((2 * xi + core) * cw + s * 2 * VDIM, 128)
        del at
        pltpu.make_async_copy(landed, landed, o_sem.at[s, xi]).wait()
        return carry

    for xi in range(nx):
        q_copy(xi).wait_send()
    for m in messages:
        copy_of(m.name).wait_send()
    lax.fori_loop(0, stages * nx, close, 0)


def shards(queries, latent, rope_keys, key_weight, value_weight, doc_lengths):
    n_seq, n_head = lax.axis_size("seq"), lax.axis_size("head")
    nx = n_head // 2
    tok, rank = latent.shape
    stages = key_weight.shape[1] // (2 * NOPE)
    docs = doc_lengths.shape[0]
    latrope = jnp.concatenate(
        [latent, rope_keys, jnp.zeros((tok, 2 * ROPE - rope_keys.shape[1]), latent.dtype)], axis=1
    )
    count = len(weight_messages(stages, nx, n_seq // NY)) + 3
    anywhere = pl.BlockSpec(memory_space=pl.ANY)
    dma = pltpu.SemaphoreType.DMA
    bf16 = jnp.bfloat16
    return pl.pallas_call(
        functools.partial(kernel, (n_seq, n_head, stages)),
        out_shape=jax.ShapeDtypeStruct((tok, n_head * stages * 2 * VDIM), bf16),
        in_specs=[anywhere] * 5,
        out_specs=anywhere,
        scratch_shapes=[
            pltpu.VMEM((4 * stages, nx, n_seq // NY, NY, key_weight.shape[0], 128), bf16),
            pltpu.VMEM((4, tok, rank + 2 * ROPE), bf16),
            pltpu.VMEM((2, nx, tok, 2 * stages * QK), bf16),
            pltpu.VMEM((2, 4 * tok, 2 * NOPE), bf16),
            pltpu.VMEM((4 * tok, 2 * ROPE), jnp.float32),
            pltpu.VMEM((4 * tok, 2 * VDIM), bf16),
            pltpu.VMEM((2 * tok, 4 * tok), jnp.float32),
            pltpu.VMEM((2, stages, nx, tok, 2 * VDIM), bf16),
            pltpu.VMEM((1, docs), jnp.int32),
            dma((stages,)),
            dma((4,)),
            dma((1,)),
            dma((3,)),
            dma((count,)),
            dma((count,)),
            dma((2, nx)),
            dma((nx,)),
            dma((stages, nx)),
            dma((stages, nx)),
            dma((stages, nx)),
        ],
        compiler_params=pltpu.CompilerParams(collective_id=0, has_side_effects=True),
    )(queries, latrope, key_weight, value_weight, doc_lengths.reshape(1, docs))


def solution(mesh):
    placed = (
        P(("seq", "head"), None),
        P(("seq", "head"), None),
        P(("seq", "head"), None),
        P("seq", "head"),
        P("seq", "head"),
        P(),
    )
    return jax.shard_map(
        shards, mesh=mesh, in_specs=placed, out_specs=P(("seq", "head"), None), check_vma=False
    )
```

```python
import functools
import math

import jax
import jax.numpy as jnp
from jax import lax
from jax.experimental import pallas as pl
from jax.experimental.pallas import tpu as pltpu
from jax.sharding import PartitionSpec as P

NOPE = 128
ROPE = 64
VDIM = 128
QK = NOPE + ROPE
LOG2E = 1.4426950408889634
NY = 4

MESH = pl.DeviceIdType.MESH

STAGES = (("x", 0), ("y", 4), ("y", 2), ("x", 4))
UNITS = 4
RATE = 46.6e3
LATENCY = 2.3
HOP = 0.8
D2D_RATE = 300e3
BACKLOG = 0.7
SEND_COST = 0.04
WAIT_COST = 0.02
LENGTH = {"first": 0.4, "both": 0.9, "last": 0.6, "setup": 0.8}
OFFSETS = (0, -1, 1, 2)


class Message:
    def __init__(self, name, group, kind, deps, link, size, priority, units=None, where=None, move=None, hops=1):
        self.name, self.group, self.kind, self.deps, self.link = name, group, kind, deps, link
        self.size, self.priority, self.units, self.where = size, priority, units, where
        self.move, self.hops = move, hops


def weight_messages(nx, nz):
    tile = 16 * 128 * 2
    half = nz // 2
    found = []

    def add(name, group, kind, deps, axis, step, units, where, priority, blocks):
        move = {"x": 0, "z": 0, "y": 0}
        move[axis] = step
        link = axis + ("+" if step > 0 else "-")
        found.append(Message(
            name, group, kind, deps, link, blocks * units[1] * tile, priority, units, where, move, abs(step)
        ))

    for s, (last, count) in enumerate(STAGES):
        minor = "y" if last == "x" else "x"
        every, far, over = (UNITS * s, UNITS), (UNITS * s, count), (UNITS * s + count, UNITS - count)

        def at(minor_at, last_at, z_at):
            return {minor: minor_at, last: last_at, "z": z_at}

        near = [(s, "near", k) for k in (1, -1, 2)]
        for k in (1, -1, 2):
            add((s, "near", k), (s, "near"), "near", [], minor, k, every, at(0, 0, 0), (0, s), 1)
        reach = {1: half - s % 2, -1: half - 1 + s % 2}
        came = {0: near}
        for way in (1, -1):
            for d in range(1, reach[way] + 1):
                deps = near if d == 1 else [(s, "z", way, d - 1)]
                name = (s, "z", way, d)
                add(name, name, "z", deps, "z", way, every, at(None, 0, -way * (d - 1)), (s, 0), 4)
                came[-way * d] = [name]
        if count:
            name = (s, "far")
            add(name, name, "far", near, last, 2, far, at(None, 0, 0), (s, 1), 4)
            for way in (1, -1):
                for d in range(1, reach[way] + 1):
                    deps = [(s, "far")] if d == 1 else [(s, "farz", way, d - 1)]
                    name = (s, "farz", way, d)
                    add(name, name, "far", deps, "z", way, far, at(None, 2, -way * (d - 1)), (s, 2), 4)
        for r, deps in came.items():
            via = 1 if r in (0, -1, -2, -3) else -1
            for way in (1, -1):
                name = (s, "side", way, r)
                relayed = way == via and count < UNITS
                group = name if relayed else (s, "side", way, "rest")
                add(name, group, "side", deps, last, way, every, at(None, 0, r), (s, 3), 4)
                if relayed:
                    add(
                        (s, "over", way, r), (s, "over", way), "over", [name], last, way, over,
                        at(None, -way, r), (s, 2), 4,
                    )
    return found


def latent_messages(tok, rank):
    size = tok * (rank + ROPE) * 2
    return [
        Message(("next",), ("next",), "latent", [], "x+", size, (0, 9), hops=1.5),
        Message(("mate",), ("mate",), "latent", [], "d2d", size, (0, 9)),
        Message(("share",), ("share",), "latent", [("next",)], "d2d", size, (0, 9)),
    ]


def step_needs(messages, s, off):
    groups = {m.group for m in messages if m.name[0] == s}
    if STAGES[s][0] == "y":
        return groups
    if off == 0:
        return {g for g in groups if g[1] in ("near", "z")}
    if off in (-1, 1):
        return {g for g in groups if g[1] == "side" and g[2] == -off}
    return {g for g in groups if g[1] in ("over", "far", "farz")}


def make_plan(messages):
    pieces = [("setup", {("next",), ("mate",), ("share",)})]
    steps = [(s, off) for s in range(len(STAGES)) for off in OFFSETS]
    for k, (s, off) in enumerate(steps):
        kind = "first" if k == 0 else "both"
        if k == len(steps) - 1:
            pieces.append((("last", k - 1), set()))
            kind = "first"
        pieces.append(((kind, k), step_needs(messages, s, off)))
    pieces.append((("last", len(steps) - 1), set()))
    group_of = {m.name: m.group for m in messages}
    left = {}
    for m in messages:
        left[m.group] = left.get(m.group, 0) + 1
    order, free, flying, seen = [], {}, [], set()
    waiting = sorted(messages, key=lambda m: m.priority)
    now, at_piece = 0.0, 0
    while waiting or flying or at_piece < len(pieces):
        flying.sort(key=lambda f: f[:2])
        if flying and flying[0][0] <= now:
            group = flying.pop(0)[2]
            left[group] -= 1
            if left[group] == 0:
                seen.add(group)
                order.append(("wait", group))
                now += WAIT_COST
            continue
        ready = [m for m in waiting if all(group_of[d] in seen for d in m.deps)]
        able = [m for m in ready if free.get(m.link, 0.0) - now < BACKLOG]
        if able:
            m = able[0]
            waiting.remove(m)
            order.append(("send", m.name))
            now += SEND_COST
            rate = D2D_RATE if m.link == "d2d" else RATE
            begun = max(now, free.get(m.link, 0.0))
            free[m.link] = begun + m.size * max(1, m.hops) / rate
            flying.append((free[m.link] + LATENCY + HOP * (m.hops - 1), len(order), m.group))
            continue
        if at_piece < len(pieces) and pieces[at_piece][1] <= seen:
            name = pieces[at_piece][0]
            order.append(("piece", name))
            now += LENGTH[name if name == "setup" else name[0]]
            at_piece += 1
            continue
        times = [f[0] for f in flying[:1]] + [free[m.link] - BACKLOG for m in ready]
        now = max(now, min(times)) + 1e-6
    return order, now


SEND_KINDS = ("near", "z", "far", "side", "over")


def kernel(
    sizes, queries, latent, rope, key_weight, value_weight, lengths, out,
    w, lat, rope_all, qbuf, kaug0, kaug1, rope_odd, vbuf0, vbuf1, bias, obuf, len_buf,
    own_sem, lat_sem, rope_sem, len_sem, lat_send, w_recv, w_send, q_sem, q_send, o_sem,
):
    n_seq, n_head, stages = sizes
    nx, ny, nz = n_head // 2, NY, n_seq // NY
    tok, rank = latent.shape
    keys = 4 * tok
    seq, head = lax.axis_index("seq"), lax.axis_index("head")
    x, core = head // 2, head % 2
    z, y = seq // ny, seq % ny
    mate = 2 * x + 1 - core
    slot = seq * nx + x
    after, before = (slot + 1) % (n_seq * nx), (slot + n_seq * nx - 1) % (n_seq * nx)

    messages = weight_messages(nx, nz)
    every = messages + latent_messages(tok, rank)
    order, _ = make_plan(every)
    by_name = {m.name: m for m in every}
    groups = list(dict.fromkeys(m.group for m in messages))
    number = {g: i for i, g in enumerate(groups)}
    members = {g: [m for m in messages if m.group == g] for g in groups}
    sent_tiles = {kind: sum(m.size for m in messages if m.kind == kind) // 4096 for kind in SEND_KINDS}

    def device(dx, dy, dz):
        return ((z + dz) % nz) * ny + (y + dy) % ny, ((x + dx) % nx) * 2 + core

    def chip(which):
        return which // nx, (which % nx) * 2 + core

    barrier = pltpu.get_barrier_semaphore()
    peers = [device(k, 0, 0) for k in range(1, nx)] + [device(0, k, 0) for k in range(1, ny)]
    peers += [device(0, 0, 1), device(0, 0, nz - 1), (seq, mate), chip(after), chip(before)]
    for peer in peers:
        pl.semaphore_signal(barrier, inc=1, device_id=peer, device_id_type=MESH)

    for s in range(stages):
        for kv, source in enumerate((key_weight, value_weight)):
            for j in range(2):
                pltpu.make_async_copy(
                    source.at[:, pl.ds((2 * s + j) * 128, 128)],
                    w.at[UNITS * s + 2 * kv + j, x, z, y], own_sem.at[0],
                ).start()
    pltpu.make_async_copy(latent, lat.at[2 + core], lat_sem.at[2 + core]).start()
    pltpu.make_async_copy(rope, rope_all.at[2 + core], rope_sem.at[2 + core]).start()
    length_copy = pltpu.make_async_copy(lengths, len_buf, len_sem.at[0])
    length_copy.start()
    qw, cw = 2 * stages * QK, 2 * stages * VDIM

    def q_part(to_core, xi):
        return queries.at[:, pl.ds(pl.multiple_of((2 * xi + to_core) * qw, 128), qw)]

    for xi in range(nx):
        pltpu.make_async_copy(q_part(core, xi), qbuf.at[core, xi], q_sem.at[core]).start()

    def tiles(count):
        a, b, c, d = w.shape[:4]
        for k in range(1, d + 1):
            for j in range(1, c + 1):
                for i in range(1, b + 1):
                    if count % (i * j * k) == 0 and count // (i * j * k) <= a:
                        return w.at[pl.ds(0, count // (i * j * k)), pl.ds(0, i), pl.ds(0, j), pl.ds(0, k)]
        raise ValueError(count)

    def await_bytes(ref, sem):
        pltpu.make_async_copy(ref, ref, sem).wait()

    await_bytes(w.at[:, x, z, y], own_sem.at[0])
    pl.semaphore_wait(barrier, len(peers))

    def place(at, here, n):
        return pl.ds(0, n) if at is None else (here + at % n) % n

    def block(m, sent):
        def shifted(a):
            at = m.where[a]
            return at if at is None or sent else at - m.move[a]

        return w.at[
            pl.ds(*m.units), place(shifted("x"), x, nx), place(shifted("z"), z, nz), place(shifted("y"), y, ny)
        ]

    def remote(src, dst, send_sem, recv_sem, to):
        return pltpu.make_async_remote_copy(
            src_ref=src, dst_ref=dst, send_sem=send_sem, recv_sem=recv_sem,
            device_id=to, device_id_type=MESH,
        )

    def latent_copies(name):
        at = 2 + core if name == ("mate",) else core
        to = chip(after) if name == ("next",) else (seq, mate)
        shared = name == ("share",)
        return [
            remote(
                held.at[at] if shared else mine, held.at[at], lat_send.at[0], sems.at[at], to
            )
            for mine, held, sems in ((latent, lat, lat_sem), (rope, rope_all, rope_sem))
        ]

    def send(name):
        m = by_name[name]
        if m.kind == "latent":
            for copy in latent_copies(name):
                copy.start()
            return
        sent = block(m, True)
        remote(
            sent, sent, w_send.at[SEND_KINDS.index(m.kind)], w_recv.at[number[m.group]],
            device(m.move["x"], m.move["y"], m.move["z"]),
        ).start()

    def lat_wait(at):
        await_bytes(lat.at[at], lat_sem.at[at])
        await_bytes(rope_all.at[at], rope_sem.at[at])

    def take(group):
        if group == ("next",):
            lat_wait(core)
        elif group == ("mate",):
            lat_wait(3 - core)
        elif group == ("share",):
            lat_wait(1 - core)
        elif len(members[group]) == 1:
            await_bytes(block(members[group][0], False), w_recv.at[number[group]])
        else:
            count = sum(m.size for m in members[group]) // 4096
            await_bytes(tiles(count), w_recv.at[number[group]])

    def q_copy(xi):
        return remote(
            q_part(1 - core, xi), qbuf.at[core, xi], q_send.at[0], q_sem.at[core], (seq, mate)
        )

    def setup():
        lat_wait(2 + core)
        length_copy.wait()
        lane = lax.broadcasted_iota(jnp.int32, (1, lengths.shape[1]), 1)
        start_own = jnp.sum(jnp.where(lane < slot, len_buf[...], 0), axis=1, keepdims=True)
        start_last = jnp.sum(jnp.where(lane < slot - 1, len_buf[...], 0), axis=1, keepdims=True)
        first = slot * 2 * tok
        q_place = first + lax.broadcasted_iota(jnp.int32, (2 * tok, 1), 0)
        begun = jnp.where(q_place >= start_own, start_own, start_last)
        k_place = first - 2 * tok + lax.broadcasted_iota(jnp.int32, (2 * tok, keys), 1)
        bias[...] = jnp.where((k_place >= begun) & (k_place <= q_place), 0.0, -jnp.inf)
        for at in range(4):
            turned = rope_all[at].astype(jnp.float32)
            tail = jnp.concatenate([turned, jnp.zeros_like(turned)], axis=0).T
            rows = slice(at * tok, (at + 1) * tok)
            for kaug in (kaug0, kaug1):
                kaug[0, rows, NOPE:] = tail.astype(jnp.bfloat16)
            rope_odd[rows, :] = pltpu.roll(tail, ROPE, axis=1)
        for t in range(2):
            await_bytes(qbuf.at[t], q_sem.at[t])

    scale = LOG2E / math.sqrt(QK)
    held = ((kaug0, vbuf0), (kaug1, vbuf1))

    def where(k):
        s, turn = k // nx, k % nx
        if isinstance(k, int):
            return s, (x + OFFSETS[turn] % nx) % nx
        off = jnp.where(turn == 0, 0, jnp.where(turn == 1, nx - 1, jnp.where(turn == 2, 1, 2)))
        return s, (x + off) % nx

    def weights(s, j, xi):
        parts = [w[UNITS * s + j + i, xi].reshape(n_seq * 16, 128) for i in range(2)]
        return jnp.concatenate(parts, axis=1)

    def project(k, parity):
        s, xi = where(k)
        kaug, vbuf = held[parity]
        tokens = lat[...].reshape(keys, rank)
        low = lax.broadcasted_iota(jnp.int32, (keys, NOPE), 1) < ROPE
        k = jnp.dot(tokens, weights(s, 0, xi), preferred_element_type=jnp.float32)
        kaug[0, :, :NOPE] = k[:, :NOPE].astype(jnp.bfloat16)
        turned = pltpu.roll(k[:, NOPE:], ROPE, axis=1)
        kaug[1, :, :NOPE] = jnp.where(low, 0.0, turned).astype(jnp.bfloat16)
        kaug[1, :, NOPE:] = jnp.where(low, turned, rope_odd[...]).astype(jnp.bfloat16)
        v = jnp.dot(tokens, weights(s, 2, xi), preferred_element_type=jnp.float32)
        vbuf[...] = v.astype(jnp.bfloat16)

    def attend(k, parity):
        s, xi = where(k)
        kaug, vbuf = held[parity]
        for t in range(2):
            span = (3 + t) * tok
            hide = bias[t * tok:(t + 1) * tok, :span]
            for h in range(2):
                begin = pl.multiple_of(s * 2 * QK + h * NOPE, 128)
                q = qbuf[t, xi, :, pl.ds(begin, 2 * NOPE)]
                sc = lax.dot_general(
                    q, kaug[h, :span, :], (((1,), (1,)), ((), ())),
                    preferred_element_type=jnp.float32,
                )
                sc = sc * scale + hide
                peak = jnp.max(sc, axis=1, keepdims=True)
                expo = jnp.exp2(sc - peak)
                total = jnp.sum(expo, axis=1, keepdims=True)
                cols = slice(h * VDIM, (h + 1) * VDIM)
                mixed = jnp.dot(
                    expo.astype(jnp.bfloat16), vbuf[:span, cols],
                    preferred_element_type=jnp.float32,
                )
                obuf[t, s, xi, :, cols] = (mixed / total).astype(jnp.bfloat16)

    def give(k):
        s, xi = where(k)
        at = pl.multiple_of((2 * xi + core) * cw + s * 2 * VDIM, 128)
        landed = out.at[:, pl.ds(at, 2 * VDIM)]
        pltpu.make_async_copy(obuf.at[core, s, xi], landed, o_sem.at[0]).start()
        remote(obuf.at[1 - core, s, xi], landed, o_sem.at[1], o_sem.at[2], (seq, mate)).start()

    def act(kind, name):
        if kind == "send":
            send(name)
        else:
            take(name)

    steps = stages * nx
    between, current = {}, "setup"
    for kind, name in [("piece", "setup")] + order:
        if kind != "piece":
            between[current].append((kind, name))
        elif name == "setup":
            current = "setup" if not between else "ready"
            between[current] = []
        else:
            current = name
            between[current] = []

    def events(name):
        for kind, what in between[name]:
            act(kind, what)

    def events_of(j, low, high, back):
        if not any(between["both", 2 * k + 1 + back] for k in range(low, high)):
            return
        if high - low == 1:
            events(("both", 2 * low + 1 + back))
            return
        middle = (low + high) // 2
        pl.when(j < middle)(functools.partial(events_of, j, low, middle, back))
        pl.when(j >= middle)(functools.partial(events_of, j, middle, high, back))

    events("setup")
    for xi in range(nx):
        q_copy(xi).start()
    setup()
    events("ready")
    project(0, 0)
    events(("first", 0))

    def pair(j, carry):
        for back in range(2):
            k = 2 * j + back
            project(k + 1, 1 - back)
            attend(k, back)
            give(k)
            events_of(j, 0, steps // 2 - 1, back)
        return carry

    lax.fori_loop(0, steps // 2 - 1, pair, 0)
    attend(steps - 2, 0)
    give(steps - 2)
    events(("last", steps - 2))
    project(steps - 1, 1)
    events(("first", steps - 1))
    attend(steps - 1, 1)
    give(steps - 1)
    events(("last", steps - 1))

    for i, kind in enumerate(SEND_KINDS):
        await_bytes(tiles(sent_tiles[kind]), w_send.at[i])
    await_bytes(tiles(3 * tok * (rank + ROPE) * 2 // 4096), lat_send.at[0])
    await_bytes(qbuf.at[core], q_send.at[0])
    await_bytes(obuf.at[core], o_sem.at[0])
    await_bytes(obuf.at[1 - core], o_sem.at[1])
    await_bytes(obuf.at[core], o_sem.at[2])


def shards(queries, latent, rope_keys, key_weight, value_weight, doc_lengths):
    n_seq, n_head = lax.axis_size("seq"), lax.axis_size("head")
    nx = n_head // 2
    tok, rank = latent.shape
    stages = key_weight.shape[1] // (2 * NOPE)
    docs = doc_lengths.shape[0]
    count = len({m.group for m in weight_messages(nx, n_seq // NY)})
    anywhere = pl.BlockSpec(memory_space=pl.ANY)
    dma = pltpu.SemaphoreType.DMA
    bf16 = jnp.bfloat16
    return pl.pallas_call(
        functools.partial(kernel, (n_seq, n_head, stages)),
        out_shape=jax.ShapeDtypeStruct((tok, n_head * stages * 2 * VDIM), bf16),
        in_specs=[anywhere] * 6,
        out_specs=anywhere,
        scratch_shapes=[
            pltpu.VMEM((UNITS * stages, nx, n_seq // NY, NY, key_weight.shape[0], 128), bf16),
            pltpu.VMEM((4, tok, rank), bf16),
            pltpu.VMEM((4, ROPE, tok), bf16),
            pltpu.VMEM((2, nx, tok, 2 * stages * QK), bf16),
            pltpu.VMEM((2, 4 * tok, 2 * NOPE), bf16),
            pltpu.VMEM((2, 4 * tok, 2 * NOPE), bf16),
            pltpu.VMEM((4 * tok, 2 * ROPE), jnp.float32),
            pltpu.VMEM((4 * tok, 2 * VDIM), bf16),
            pltpu.VMEM((4 * tok, 2 * VDIM), bf16),
            pltpu.VMEM((2 * tok, 4 * tok), jnp.float32),
            pltpu.VMEM((2, stages, nx, tok, 2 * VDIM), bf16),
            pltpu.VMEM((1, docs), jnp.int32),
            dma((1,)),
            dma((4,)),
            dma((4,)),
            dma((1,)),
            dma((1,)),
            dma((count,)),
            dma((len(SEND_KINDS),)),
            dma((2,)),
            dma((1,)),
            dma((3,)),
        ],
        compiler_params=pltpu.CompilerParams(collective_id=0, has_side_effects=True),
    )(queries, latent, rope_keys.T, key_weight, value_weight, doc_lengths.reshape(1, docs))


def solution(mesh):
    placed = (
        P(("seq", "head"), None),
        P(("seq", "head"), None),
        P(("seq", "head"), None),
        P("seq", "head"),
        P("seq", "head"),
        P(),
    )
    return jax.shard_map(
        shards, mesh=mesh, in_specs=placed, out_specs=P(("seq", "head"), None), check_vma=False
    )
```

```python
import functools
import math

import jax
import jax.numpy as jnp
from jax import lax
from jax.experimental import pallas as pl
from jax.experimental.pallas import tpu as pltpu
from jax.sharding import PartitionSpec as P

NOPE = 128
ROPE = 64
VDIM = 128
QK = NOPE + ROPE
LOG2E = 1.4426950408889634
NY = 4

MESH = pl.DeviceIdType.MESH

STAGES = (("x", 0), ("y", 4), ("y", 2), ("x", 4))
UNITS = 4
RATE = 46.6e3
LATENCY = 2.3
HOP = 0.8
D2D_RATE = 300e3
BACKLOG = 0.7
SEND_COST = 0.04
WAIT_COST = 0.02
LENGTH = {"block": 0.8, "setup": 0.8}
DEPTH = 3
OFFSETS = (0, -1, 1, 2)
CHUNK = 32


class Message:
    def __init__(self, name, group, kind, deps, link, size, priority, units=None, where=None, move=None, hops=1):
        self.name, self.group, self.kind, self.deps, self.link = name, group, kind, deps, link
        self.size, self.priority, self.units, self.where = size, priority, units, where
        self.move, self.hops = move, hops


def weight_messages(nx, nz):
    tile = 16 * 128 * 2
    half = nz // 2
    found = []

    def add(name, group, kind, deps, axis, step, units, where, priority, blocks):
        move = {"x": 0, "z": 0, "y": 0}
        move[axis] = step
        link = axis + ("+" if step > 0 else "-")
        found.append(Message(
            name, group, kind, deps, link, blocks * units[1] * tile, priority, units, where, move, abs(step)
        ))

    for s, (last, count) in enumerate(STAGES):
        minor = "y" if last == "x" else "x"
        every, far, over = (UNITS * s, UNITS), (UNITS * s, count), (UNITS * s + count, UNITS - count)

        def at(minor_at, last_at, z_at):
            return {minor: minor_at, last: last_at, "z": z_at}

        near = [(s, "near", k) for k in (1, -1, 2)]
        for k in (1, -1, 2):
            add((s, "near", k), (s, "near"), "near", [], minor, k, every, at(0, 0, 0), (0, s), 1)
        reach = {1: half - s % 2, -1: half - 1 + s % 2}
        came = {0: near}
        for way in (1, -1):
            for d in range(1, reach[way] + 1):
                deps = near if d == 1 else [(s, "z", way, d - 1)]
                name = (s, "z", way, d)
                add(name, name, "z", deps, "z", way, every, at(None, 0, -way * (d - 1)), (s, 0), 4)
                came[-way * d] = [name]
        if count:
            name = (s, "far")
            add(name, name, "far", near, last, 2, far, at(None, 0, 0), (s, 1), 4)
            for way in (1, -1):
                for d in range(1, reach[way] + 1):
                    deps = [(s, "far")] if d == 1 else [(s, "farz", way, d - 1)]
                    name = (s, "farz", way, d)
                    add(name, name, "far", deps, "z", way, far, at(None, 2, -way * (d - 1)), (s, 2), 4)
        for r, deps in came.items():
            via = 1 if r in (0, -1, -2, -3) else -1
            for way in (1, -1):
                name = (s, "side", way, r)
                relayed = way == via and count < UNITS
                group = name if relayed else (s, "side", way, "rest")
                add(name, group, "side", deps, last, way, every, at(None, 0, r), (s, 3), 4)
                if relayed:
                    add(
                        (s, "over", way, r), (s, "over", way), "over", [name], last, way, over,
                        at(None, -way, r), (s, 2), 4,
                    )
    return found


def latent_messages(tok, rank):
    size = tok * (rank + ROPE) * 2
    return [
        Message(("next",), ("next",), "latent", [], "x+", size, (0, 9), hops=1.5),
        Message(("mate",), ("mate",), "latent", [], "d2d", size, (0, 9)),
        Message(("share",), ("share",), "latent", [("next",)], "d2d", size, (0, 9)),
    ]


def step_needs(messages, s, off):
    groups = {m.group for m in messages if m.name[0] == s}
    if STAGES[s][0] == "y":
        return groups
    if off == 0:
        return {g for g in groups if g[1] in ("near", "z")}
    if off in (-1, 1):
        return {g for g in groups if g[1] == "side" and g[2] == -off}
    return {g for g in groups if g[1] in ("over", "far", "farz")}


def make_plan(messages):
    pieces = [("setup", {("next",), ("mate",), ("share",)})]
    steps = [(s, off) for s in range(len(STAGES)) for off in OFFSETS]
    for b in range(len(steps) + DEPTH):
        needed = step_needs(messages, *steps[b]) if b < len(steps) else set()
        pieces.append((("block", b), needed))
    group_of = {m.name: m.group for m in messages}
    left = {}
    for m in messages:
        left[m.group] = left.get(m.group, 0) + 1
    order, free, flying, seen = [], {}, [], set()
    waiting = sorted(messages, key=lambda m: m.priority)
    now, at_piece = 0.0, 0
    while waiting or flying or at_piece < len(pieces):
        flying.sort(key=lambda f: f[:2])
        if flying and flying[0][0] <= now:
            group = flying.pop(0)[2]
            left[group] -= 1
            if left[group] == 0:
                seen.add(group)
                order.append(("wait", group))
                now += WAIT_COST
            continue
        ready = [m for m in waiting if all(group_of[d] in seen for d in m.deps)]
        able = [m for m in ready if free.get(m.link, 0.0) - now < BACKLOG]
        if able:
            m = able[0]
            waiting.remove(m)
            order.append(("send", m.name))
            now += SEND_COST
            rate = D2D_RATE if m.link == "d2d" else RATE
            begun = max(now, free.get(m.link, 0.0))
            free[m.link] = begun + m.size * max(1, m.hops) / rate
            flying.append((free[m.link] + LATENCY + HOP * (m.hops - 1), len(order), m.group))
            continue
        if at_piece < len(pieces) and pieces[at_piece][1] <= seen:
            name = pieces[at_piece][0]
            order.append(("piece", name))
            now += LENGTH[name if name == "setup" else name[0]]
            at_piece += 1
            continue
        times = [f[0] for f in flying[:1]] + [free[m.link] - BACKLOG for m in ready]
        now = max(now, min(times)) + 1e-6
    return order, now


SEND_KINDS = ("near", "z", "far", "side", "over")


def kernel(
    sizes, queries, latent, rope, key_weight, value_weight, lengths, out,
    w, lat, rope_all, qbuf, kaug0, kaug1, rope_odd, vbuf0, vbuf1, sbuf0, sbuf1, pbuf0, pbuf1,
    inv0, inv1, bias, obuf, len_buf,
    own_sem, lat_sem, rope_sem, len_sem, lat_send, w_recv, w_send, q_sem, q_send, o_sem,
):
    n_seq, n_head, stages = sizes
    nx, ny, nz = n_head // 2, NY, n_seq // NY
    tok, rank = latent.shape
    keys = 4 * tok
    seq, head = lax.axis_index("seq"), lax.axis_index("head")
    x, core = head // 2, head % 2
    z, y = seq // ny, seq % ny
    mate = 2 * x + 1 - core
    slot = seq * nx + x
    after, before = (slot + 1) % (n_seq * nx), (slot + n_seq * nx - 1) % (n_seq * nx)

    messages = weight_messages(nx, nz)
    every = messages + latent_messages(tok, rank)
    order, _ = make_plan(every)
    by_name = {m.name: m for m in every}
    groups = list(dict.fromkeys(m.group for m in messages))
    number = {g: i for i, g in enumerate(groups)}
    members = {g: [m for m in messages if m.group == g] for g in groups}
    sent_tiles = {kind: sum(m.size for m in messages if m.kind == kind) // 4096 for kind in SEND_KINDS}

    def device(dx, dy, dz):
        return ((z + dz) % nz) * ny + (y + dy) % ny, ((x + dx) % nx) * 2 + core

    def chip(which):
        return which // nx, (which % nx) * 2 + core

    barrier = pltpu.get_barrier_semaphore()
    peers = [device(k, 0, 0) for k in range(1, nx)] + [device(0, k, 0) for k in range(1, ny)]
    peers += [device(0, 0, 1), device(0, 0, nz - 1), (seq, mate), chip(after), chip(before)]
    for peer in peers:
        pl.semaphore_signal(barrier, inc=1, device_id=peer, device_id_type=MESH)

    for s in range(stages):
        for kv, source in enumerate((key_weight, value_weight)):
            for j in range(2):
                pltpu.make_async_copy(
                    source.at[:, pl.ds((2 * s + j) * 128, 128)],
                    w.at[UNITS * s + 2 * kv + j, x, z, y], own_sem.at[0],
                ).start()
    pltpu.make_async_copy(latent, lat.at[2 + core], lat_sem.at[2 + core]).start()
    pltpu.make_async_copy(rope, rope_all.at[2 + core], rope_sem.at[2 + core]).start()
    length_copy = pltpu.make_async_copy(lengths, len_buf, len_sem.at[0])
    length_copy.start()
    qw, cw = 2 * stages * QK, 2 * stages * VDIM

    def q_part(to_core, xi):
        return queries.at[:, pl.ds(pl.multiple_of((2 * xi + to_core) * qw, 128), qw)]

    for xi in range(nx):
        pltpu.make_async_copy(q_part(core, xi), qbuf.at[core, xi], q_sem.at[core]).start()

    def tiles(count):
        a, b, c, d = w.shape[:4]
        for k in range(1, d + 1):
            for j in range(1, c + 1):
                for i in range(1, b + 1):
                    if count % (i * j * k) == 0 and count // (i * j * k) <= a:
                        return w.at[pl.ds(0, count // (i * j * k)), pl.ds(0, i), pl.ds(0, j), pl.ds(0, k)]
        raise ValueError(count)

    def await_bytes(ref, sem):
        pltpu.make_async_copy(ref, ref, sem).wait()

    await_bytes(w.at[:, x, z, y], own_sem.at[0])
    pl.semaphore_wait(barrier, len(peers))

    def place(at, here, n):
        return pl.ds(0, n) if at is None else (here + at % n) % n

    def block(m, sent):
        def shifted(a):
            at = m.where[a]
            return at if at is None or sent else at - m.move[a]

        return w.at[
            pl.ds(*m.units), place(shifted("x"), x, nx), place(shifted("z"), z, nz), place(shifted("y"), y, ny)
        ]

    def remote(src, dst, send_sem, recv_sem, to):
        return pltpu.make_async_remote_copy(
            src_ref=src, dst_ref=dst, send_sem=send_sem, recv_sem=recv_sem,
            device_id=to, device_id_type=MESH,
        )

    def latent_copies(name):
        at = 2 + core if name == ("mate",) else core
        to = chip(after) if name == ("next",) else (seq, mate)
        shared = name == ("share",)
        return [
            remote(
                held.at[at] if shared else mine, held.at[at], lat_send.at[0], sems.at[at], to
            )
            for mine, held, sems in ((latent, lat, lat_sem), (rope, rope_all, rope_sem))
        ]

    def send(name):
        m = by_name[name]
        if m.kind == "latent":
            for copy in latent_copies(name):
                copy.start()
            return
        sent = block(m, True)
        remote(
            sent, sent, w_send.at[SEND_KINDS.index(m.kind)], w_recv.at[number[m.group]],
            device(m.move["x"], m.move["y"], m.move["z"]),
        ).start()

    def lat_wait(at):
        await_bytes(lat.at[at], lat_sem.at[at])
        await_bytes(rope_all.at[at], rope_sem.at[at])

    def take(group):
        if group == ("next",):
            lat_wait(core)
        elif group == ("mate",):
            lat_wait(3 - core)
        elif group == ("share",):
            lat_wait(1 - core)
        elif len(members[group]) == 1:
            await_bytes(block(members[group][0], False), w_recv.at[number[group]])
        else:
            count = sum(m.size for m in members[group]) // 4096
            await_bytes(tiles(count), w_recv.at[number[group]])

    def q_copy(xi):
        return remote(
            q_part(1 - core, xi), qbuf.at[core, xi], q_send.at[0], q_sem.at[core], (seq, mate)
        )

    def setup():
        lat_wait(2 + core)
        length_copy.wait()
        lane = lax.broadcasted_iota(jnp.int32, (1, lengths.shape[1]), 1)
        start_own = jnp.sum(jnp.where(lane < slot, len_buf[...], 0), axis=1, keepdims=True)
        start_last = jnp.sum(jnp.where(lane < slot - 1, len_buf[...], 0), axis=1, keepdims=True)
        first = slot * 2 * tok
        q_place = first + lax.broadcasted_iota(jnp.int32, (2 * tok, 1), 0)
        begun = jnp.where(q_place >= start_own, start_own, start_last)
        k_place = first - 2 * tok + lax.broadcasted_iota(jnp.int32, (2 * tok, keys), 1)
        bias[...] = jnp.where((k_place >= begun) & (k_place <= q_place), 0.0, -jnp.inf)
        for at in range(4):
            turned = rope_all[at].astype(jnp.float32)
            tail = jnp.concatenate([turned, jnp.zeros_like(turned)], axis=0).T
            rows = slice(at * tok, (at + 1) * tok)
            for kaug in (kaug0, kaug1):
                kaug[0, rows, NOPE:] = tail.astype(jnp.bfloat16)
            rope_odd[rows, :] = pltpu.roll(tail, ROPE, axis=1)
        for pbuf in (pbuf0, pbuf1):
            pbuf[:, :tok, 3 * tok:] = jnp.zeros((2, tok, tok), jnp.bfloat16)
        for t in range(2):
            await_bytes(qbuf.at[t], q_sem.at[t])

    scale = LOG2E / math.sqrt(QK)
    held = ((kaug0, vbuf0, sbuf0, pbuf0, inv0), (kaug1, vbuf1, sbuf1, pbuf1, inv1))

    def where(k):
        s, turn = k // nx, k % nx
        if isinstance(k, int):
            return s, (x + OFFSETS[turn] % nx) % nx
        off = jnp.where(turn == 0, 0, jnp.where(turn == 1, nx - 1, jnp.where(turn == 2, 1, 2)))
        return s, (x + off) % nx

    def weights(s, j, xi):
        parts = [w[UNITS * s + j + i, xi].reshape(n_seq * 16, 128) for i in range(2)]
        return jnp.concatenate(parts, axis=1)

    def project_keys(k, parity):
        s, xi = where(k)
        kaug = held[parity][0]
        low = lax.broadcasted_iota(jnp.int32, (keys, NOPE), 1) < ROPE
        k = jnp.dot(lat[...].reshape(keys, rank), weights(s, 0, xi), preferred_element_type=jnp.float32)
        kaug[0, :, :NOPE] = k[:, :NOPE].astype(jnp.bfloat16)
        turned = pltpu.roll(k[:, NOPE:], ROPE, axis=1)
        kaug[1, :, :NOPE] = jnp.where(low, 0.0, turned).astype(jnp.bfloat16)
        kaug[1, :, NOPE:] = jnp.where(low, turned, rope_odd[...]).astype(jnp.bfloat16)

    def project_values(k, parity):
        s, xi = where(k)
        v = jnp.dot(lat[...].reshape(keys, rank), weights(s, 2, xi), preferred_element_type=jnp.float32)
        held[parity][1][...] = v.astype(jnp.bfloat16)

    def score(k, parity):
        s, xi = where(k)
        kaug, _, sbuf, _, _ = held[parity]
        for h in range(2):
            begin = pl.multiple_of(s * 2 * QK + h * NOPE, 128)
            q = qbuf[:, xi, :, pl.ds(begin, 2 * NOPE)].reshape(2 * tok, 2 * NOPE)
            sc = lax.dot_general(
                q, kaug[h], (((1,), (1,)), ((), ())), preferred_element_type=jnp.float32
            )
            for t in range(2):
                rows, span = slice(t * tok, (t + 1) * tok), (3 + t) * tok
                sbuf[h, rows, :span] = sc[rows, :span] * scale + bias[rows, :span]

    def soften(parity):
        _, _, sbuf, pbuf, inv = held[parity]
        for t in range(2):
            span = (3 + t) * tok
            for h in range(2):
                for r in range(0, tok, CHUNK):
                    rows = slice(t * tok + r, t * tok + r + CHUNK)
                    sc = sbuf[h, rows, :span]
                    expo = jnp.exp2(sc - jnp.max(sc, axis=1, keepdims=True))
                    total = jnp.sum(expo, axis=1, keepdims=True)
                    inv[h, rows, :] = jnp.broadcast_to(1.0 / total, (CHUNK, VDIM))
                    pbuf[h, rows, :span] = expo.astype(jnp.bfloat16)

    def mix(k, parity):
        s, xi = where(k)
        _, vbuf, _, pbuf, inv = held[parity]
        for h in range(2):
            cols = slice(h * VDIM, (h + 1) * VDIM)
            mixed = jnp.dot(pbuf[h], vbuf[:, cols], preferred_element_type=jnp.float32)
            mixed = (mixed * inv[h]).astype(jnp.bfloat16)
            for t in range(2):
                obuf[t, s, xi, :, cols] = mixed[t * tok:(t + 1) * tok]

    def give(k):
        s, xi = where(k)
        at = pl.multiple_of((2 * xi + core) * cw + s * 2 * VDIM, 128)
        landed = out.at[:, pl.ds(at, 2 * VDIM)]
        pltpu.make_async_copy(obuf.at[core, s, xi], landed, o_sem.at[0]).start()
        remote(obuf.at[1 - core, s, xi], landed, o_sem.at[1], o_sem.at[2], (seq, mate)).start()

    def act(kind, name):
        if kind == "send":
            send(name)
        else:
            take(name)

    steps = stages * nx
    between, current = {}, "setup"
    for kind, name in [("piece", "setup")] + order:
        if kind != "piece":
            between[current].append((kind, name))
        elif name == "setup":
            current = "setup" if not between else "ready"
            between[current] = []
        else:
            current = name
            between[current] = []

    def events(name):
        for kind, what in between[name]:
            act(kind, what)

    def events_of(j, low, high, back):
        if not any(between["block", DEPTH + 2 * k + back] for k in range(low, high)):
            return
        if high - low == 1:
            events(("block", DEPTH + 2 * low + back))
            return
        middle = (low + high) // 2
        pl.when(j < middle)(functools.partial(events_of, j, low, middle, back))
        pl.when(j >= middle)(functools.partial(events_of, j, middle, high, back))

    def run(b, turn, first, last):
        if first <= 1 <= last:
            score(b - 1, (turn - 1) % 2)
        if first <= 2 <= last:
            soften(turn % 2)
        if first <= 0 <= last:
            project_keys(b, turn % 2)
        if first <= 2 <= last:
            project_values(b - 2, turn % 2)
        if first <= 3 <= last:
            mix(b - 3, (turn - 3) % 2)
            give(b - 3)

    events("setup")
    for xi in range(nx):
        q_copy(xi).start()
    setup()
    events("ready")
    for b in range(DEPTH):
        run(b, b, 0, b)
        events(("block", b))
    pairs = (steps - DEPTH) // 2

    def pair(j, carry):
        for back in range(2):
            run(DEPTH + 2 * j + back, DEPTH + back, 0, DEPTH)
            events_of(j, 0, pairs, back)
        return carry

    lax.fori_loop(0, pairs, pair, 0)
    for b in range(DEPTH + 2 * pairs, steps + DEPTH):
        run(b, b, max(0, b - steps + 1), DEPTH)
        events(("block", b))

    for i, kind in enumerate(SEND_KINDS):
        await_bytes(tiles(sent_tiles[kind]), w_send.at[i])
    await_bytes(tiles(3 * tok * (rank + ROPE) * 2 // 4096), lat_send.at[0])
    await_bytes(qbuf.at[core], q_send.at[0])
    await_bytes(obuf.at[core], o_sem.at[0])
    await_bytes(obuf.at[1 - core], o_sem.at[1])
    await_bytes(obuf.at[core], o_sem.at[2])


def shards(queries, latent, rope_keys, key_weight, value_weight, doc_lengths):
    n_seq, n_head = lax.axis_size("seq"), lax.axis_size("head")
    nx = n_head // 2
    tok, rank = latent.shape
    stages = key_weight.shape[1] // (2 * NOPE)
    docs = doc_lengths.shape[0]
    count = len({m.group for m in weight_messages(nx, n_seq // NY)})
    anywhere = pl.BlockSpec(memory_space=pl.ANY)
    dma = pltpu.SemaphoreType.DMA
    bf16 = jnp.bfloat16
    return pl.pallas_call(
        functools.partial(kernel, (n_seq, n_head, stages)),
        out_shape=jax.ShapeDtypeStruct((tok, n_head * stages * 2 * VDIM), bf16),
        in_specs=[anywhere] * 6,
        out_specs=anywhere,
        scratch_shapes=[
            pltpu.VMEM((UNITS * stages, nx, n_seq // NY, NY, key_weight.shape[0], 128), bf16),
            pltpu.VMEM((4, tok, rank), bf16),
            pltpu.VMEM((4, ROPE, tok), bf16),
            pltpu.VMEM((2, nx, tok, 2 * stages * QK), bf16),
            pltpu.VMEM((2, 4 * tok, 2 * NOPE), bf16),
            pltpu.VMEM((2, 4 * tok, 2 * NOPE), bf16),
            pltpu.VMEM((4 * tok, 2 * ROPE), jnp.float32),
            pltpu.VMEM((4 * tok, 2 * VDIM), bf16),
            pltpu.VMEM((4 * tok, 2 * VDIM), bf16),
            pltpu.VMEM((2, 2 * tok, 4 * tok), jnp.float32),
            pltpu.VMEM((2, 2 * tok, 4 * tok), jnp.float32),
            pltpu.VMEM((2, 2 * tok, 4 * tok), bf16),
            pltpu.VMEM((2, 2 * tok, 4 * tok), bf16),
            pltpu.VMEM((2, 2 * tok, VDIM), jnp.float32),
            pltpu.VMEM((2, 2 * tok, VDIM), jnp.float32),
            pltpu.VMEM((2 * tok, 4 * tok), jnp.float32),
            pltpu.VMEM((2, stages, nx, tok, 2 * VDIM), bf16),
            pltpu.VMEM((1, docs), jnp.int32),
            dma((1,)),
            dma((4,)),
            dma((4,)),
            dma((1,)),
            dma((1,)),
            dma((count,)),
            dma((len(SEND_KINDS),)),
            dma((2,)),
            dma((1,)),
            dma((3,)),
        ],
        compiler_params=pltpu.CompilerParams(collective_id=0, has_side_effects=True),
    )(queries, latent, rope_keys.T, key_weight, value_weight, doc_lengths.reshape(1, docs))


def solution(mesh):
    placed = (
        P(("seq", "head"), None),
        P(("seq", "head"), None),
        P(("seq", "head"), None),
        P("seq", "head"),
        P("seq", "head"),
        P(),
    )
    return jax.shard_map(
        shards, mesh=mesh, in_specs=placed, out_specs=P(("seq", "head"), None), check_vma=False
    )
```

```python
import collections
import functools
import math

import jax
import jax.numpy as jnp
from jax import lax
from jax.experimental import pallas as pl
from jax.experimental.pallas import tpu as pltpu
from jax.sharding import PartitionSpec as P

NOPE = 128
ROPE = 64
VDIM = 128
QK = NOPE + ROPE
LOG2E = 1.4426950408889634
NY = 4

MESH = pl.DeviceIdType.MESH

Stage = collections.namedtuple(
    "Stage", ("last", "far", "near_way", "far_way", "upwards", "split_side", "split_z")
)
STAGES = (
    Stage('x', 4, 0, -1, 1, 0, 0),
    Stage('y', 0, 0, 0, 4, 0, 1),
    Stage('y', 4, 0, -1, 6, 0, 1),
    Stage('x', 0, 0, 1, 4, 0, 0),
)
RANKS = (
    dict(near=11, z=4, far=7, farz=17, over=23, side=2),
    dict(near=6, z=0, far=9, farz=1, over=13, side=18),
    dict(near=12, z=21, far=19, farz=3, over=10, side=20),
    dict(near=16, z=14, far=24, farz=8, over=22, side=5),
)
LATENT_RANK = 15
UNITS = 4
RATE = 46.6e3
LATENCY = 3.0
HOP = 0.8
D2D_RATE = 300e3
BACKLOG = 1.0
SEND_COST = 0.04
WAIT_COST = 0.02
BLOCK = 0.8
DRAIN = (0.6, 0.5, 0.35)
DEPTH = 3
OFFSETS = (0, -1, 1, 2)
CHUNK = 32


class Message:
    def __init__(self, name, group, kind, deps, link, size, priority, units=None, where=None, move=None, hops=1):
        self.name, self.group, self.kind, self.deps, self.link = name, group, kind, deps, link
        self.size, self.priority, self.units, self.where = size, priority, units, where
        self.move, self.hops = move, hops


def weight_messages(nx, nz):
    tile = 16 * 128 * 2
    half = nz // 2
    found = []

    def add(name, group, kind, deps, axis, step, units, where, blocks):
        move = {"x": 0, "z": 0, "y": 0}
        move[axis] = step
        link = axis + ("+" if step > 0 else "-")
        rank = RANKS[name[0]][name[1]]
        found.append(Message(
            name, group, kind, deps, link, blocks * units[1] * tile, rank, units, where, move, abs(step)
        ))

    for s, stage in enumerate(STAGES):
        last, minor = stage.last, "y" if stage.last == "x" else "x"
        every, far = (UNITS * s, UNITS), (UNITS * s, stage.far)
        over = (UNITS * s + stage.far, UNITS - stage.far)

        def at(minor_at, last_at, z_at):
            return {minor: minor_at, last: last_at, "z": z_at}

        near = {k: (s, "near", k) for k in (1, -1, 2)}
        one_by_one = stage.near_way or stage.split_side or stage.split_z
        for k, name in near.items():
            group = name if one_by_one else (s, "near")
            if k == 2 and stage.near_way:
                way = stage.near_way
                add(name, group, "near", [near[way]], minor, way, every, at(-way, 0, 0), 1)
            else:
                add(name, group, "near", [], minor, k, every, at(0, 0, 0), 1)
        near = list(near.values())

        def first(name, group, kind, split, axis, way):
            if not split:
                add(name, group, kind, near, axis, way, every, at(None, 0, 0), 4)
                return [name]
            for k in (0, 1, -1, 2):
                add((*name, k), group, kind, [(s, "near", k)] if k else [], axis, way, every, at(-k, 0, 0), 1)
            return [(*name, k) for k in (0, 1, -1, 2)]

        reach = {1: half - s % 2, -1: half - 1 + s % 2}
        came = {0: near}
        for way in (1, -1):
            for d in range(1, reach[way] + 1):
                name = (s, "z", way, d)
                if d == 1:
                    came[-way] = first(name, name, "z", stage.split_z, "z", way)
                else:
                    add(name, name, "z", came[way * (1 - d)], "z", way, every, at(None, 0, way * (1 - d)), 4)
                    came[-way * d] = [name]
        if stage.far:
            name, way = (s, "far"), stage.far_way
            if way:
                deps = [(s, "side", way, 0, k) for k in (0, 1, -1, 2)] if stage.split_side else [(s, "side", way, 0)]
                add(name, name, "far", deps, last, way, far, at(None, -way, 0), 4)
            else:
                add(name, name, "far", near, last, 2, far, at(None, 0, 0), 4)
            for way in (1, -1):
                for d in range(1, reach[way] + 1):
                    deps = [(s, "far")] if d == 1 else [(s, "farz", way, d - 1)]
                    name = (s, "farz", way, d)
                    add(name, name, "far", deps, "z", way, far, at(None, 2, way * (1 - d)), 4)
        opposite = -half if s % 2 == 0 else half
        for i, r in enumerate((*range(0, -half, -1), opposite, *range(half - 1, 0, -1))):
            via = 1 if i < stage.upwards else -1
            for way in (1, -1):
                name = (s, "side", way, r)
                relayed = way == via and stage.far < UNITS
                alone = relayed or (r == 0 and stage.far and stage.far_way == way)
                group = name if alone else (s, "side", way, "rest")
                if r == 0:
                    names = first(name, group, "side", stage.split_side, last, way)
                else:
                    add(name, group, "side", came[r], last, way, every, at(None, 0, r), 4)
                    names = [name]
                if relayed:
                    deps = names
            if stage.far < UNITS:
                add((s, "over", via, r), (s, "over", via), "over", deps, last, via, over, at(None, -via, r), 4)
    return found


def latent_messages(tok, rank):
    size = tok * (rank + ROPE) * 2
    return [
        Message(("next",), ("next",), "latent", [], "x+", 1.3 * size, LATENT_RANK, hops=2),
        Message(("mate",), ("mate",), "latent", [], "d2d", size, LATENT_RANK),
        Message(("share",), ("share",), "latent", [("next",)], "d2d", size, LATENT_RANK),
    ]


def step_needs(messages, s, off):
    groups = {m.group for m in messages if m.name[0] == s}
    if STAGES[s].last == "y":
        return groups
    if off == 0:
        return {g for g in groups if g[1] in ("near", "z")}
    if off in (-1, 1):
        return {g for g in groups if g[1] == "side" and g[2] == -off}
    return {g for g in groups if g[1] in ("over", "far", "farz")}


def make_plan(messages):
    needs = {(s, off): step_needs(messages, s, off) for s in range(len(STAGES)) for off in OFFSETS}
    steps, able_steps, drained, prepared = [], [], 0, False
    group_of = {m.name: m.group for m in messages}
    left = {}
    for m in messages:
        left[m.group] = left.get(m.group, 0) + 1
    order, free, flying, seen = [], {}, [], set()
    waiting = sorted(messages, key=lambda m: m.priority)
    now = 0.0
    while waiting or flying or drained < DEPTH:
        flying.sort(key=lambda f: f[:2])
        if flying and flying[0][0] <= now:
            group = flying.pop(0)[2]
            left[group] -= 1
            if left[group] == 0:
                seen.add(group)
                order.append(("wait", group))
                now += WAIT_COST
                for step in [step for step, needed in needs.items() if needed <= seen]:
                    able_steps.append(step)
                    del needs[step]
            continue
        ready = [m for m in waiting if all(group_of[d] in seen for d in m.deps)]
        able = [m for m in ready if free.get(m.link, 0.0) - now < BACKLOG]
        if able:
            m = able[0]
            waiting.remove(m)
            order.append(("send", m.name))
            now += SEND_COST
            rate = D2D_RATE if m.link == "d2d" else RATE
            begun = max(now, free.get(m.link, 0.0))
            free[m.link] = begun + m.size * max(1, m.hops) / rate
            flying.append((free[m.link] + LATENCY + HOP * (m.hops - 1), len(order), m.group))
            continue
        if not prepared:
            if {("next",), ("mate",), ("share",)} <= seen:
                order.append(("piece", "setup"))
                now += BLOCK
                prepared = True
                continue
        elif able_steps:
            order.append(("piece", ("block", len(steps))))
            steps.append(able_steps.pop(0))
            now += BLOCK
            continue
        elif not needs and drained < DEPTH:
            order.append(("piece", ("block", len(steps) + drained)))
            now += DRAIN[drained]
            drained += 1
            continue
        times = [f[0] for f in flying[:1]] + [free[m.link] - BACKLOG for m in ready]
        now = max(now, min(times)) + 1e-6
    return order, steps, now


SEND_KINDS = ("near", "z", "far", "side", "over")


def kernel(
    sizes, queries, latent, rope, key_weight, value_weight, lengths, out,
    w, lat, rope_all, qbuf, kaug0, kaug1, rope_odd, vbuf0, vbuf1, sbuf0, sbuf1, pbuf0, pbuf1,
    inv0, inv1, bias, obuf, len_buf,
    own_sem, lat_sem, rope_sem, len_sem, lat_send, w_recv, w_send, q_sem, q_send, o_sem,
):
    n_seq, n_head, stages = sizes
    nx, ny, nz = n_head // 2, NY, n_seq // NY
    tok, rank = latent.shape
    keys = 4 * tok
    seq, head = lax.axis_index("seq"), lax.axis_index("head")
    x, core = head // 2, head % 2
    z, y = seq // ny, seq % ny
    mate = 2 * x + 1 - core
    slot = seq * nx + x
    after, before = (slot + 1) % (n_seq * nx), (slot + n_seq * nx - 1) % (n_seq * nx)

    messages = weight_messages(nx, nz)
    every = messages + latent_messages(tok, rank)
    order, turns, _ = make_plan(every)
    by_name = {m.name: m for m in every}
    groups = list(dict.fromkeys(m.group for m in messages))
    number = {g: i for i, g in enumerate(groups)}
    members = {g: [m for m in messages if m.group == g] for g in groups}
    sent_tiles = {kind: sum(m.size for m in messages if m.kind == kind) // 4096 for kind in SEND_KINDS}

    def device(dx, dy, dz):
        return ((z + dz) % nz) * ny + (y + dy) % ny, ((x + dx) % nx) * 2 + core

    def chip(which):
        return which // nx, (which % nx) * 2 + core

    barrier = pltpu.get_barrier_semaphore()
    peers = [device(k, 0, 0) for k in range(1, nx)] + [device(0, k, 0) for k in range(1, ny)]
    peers += [device(0, 0, 1), device(0, 0, nz - 1), (seq, mate), chip(after), chip(before)]
    for peer in peers:
        pl.semaphore_signal(barrier, inc=1, device_id=peer, device_id_type=MESH)

    for s in range(stages):
        for kv, source in enumerate((key_weight, value_weight)):
            for j in range(2):
                pltpu.make_async_copy(
                    source.at[:, pl.ds((2 * s + j) * 128, 128)],
                    w.at[UNITS * s + 2 * kv + j, x, z, y], own_sem.at[0],
                ).start()
    pltpu.make_async_copy(latent, lat.at[2 + core], lat_sem.at[2 + core]).start()
    pltpu.make_async_copy(rope, rope_all.at[2 + core], rope_sem.at[2 + core]).start()
    length_copy = pltpu.make_async_copy(lengths, len_buf, len_sem.at[0])
    length_copy.start()
    qw, cw = 2 * stages * QK, 2 * stages * VDIM

    def q_part(to_core, xi):
        return queries.at[:, pl.ds(pl.multiple_of((2 * xi + to_core) * qw, 128), qw)]

    for xi in range(nx):
        pltpu.make_async_copy(q_part(core, xi), qbuf.at[core, xi], q_sem.at[core]).start()

    def tiles(count):
        a, b, c, d = w.shape[:4]
        for k in range(1, d + 1):
            for j in range(1, c + 1):
                for i in range(1, b + 1):
                    if count % (i * j * k) == 0 and count // (i * j * k) <= a:
                        return w.at[pl.ds(0, count // (i * j * k)), pl.ds(0, i), pl.ds(0, j), pl.ds(0, k)]
        raise ValueError(count)

    def await_bytes(ref, sem):
        pltpu.make_async_copy(ref, ref, sem).wait()

    await_bytes(w.at[:, x, z, y], own_sem.at[0])
    pl.semaphore_wait(barrier, len(peers))

    def place(at, here, n):
        return pl.ds(0, n) if at is None else (here + at % n) % n

    def block(m, sent):
        def shifted(a):
            at = m.where[a]
            return at if at is None or sent else at - m.move[a]

        return w.at[
            pl.ds(*m.units), place(shifted("x"), x, nx), place(shifted("z"), z, nz), place(shifted("y"), y, ny)
        ]

    def remote(src, dst, send_sem, recv_sem, to):
        return pltpu.make_async_remote_copy(
            src_ref=src, dst_ref=dst, send_sem=send_sem, recv_sem=recv_sem,
            device_id=to, device_id_type=MESH,
        )

    def latent_copies(name):
        at = 2 + core if name == ("mate",) else core
        to = chip(after) if name == ("next",) else (seq, mate)
        shared = name == ("share",)
        return [
            remote(
                held.at[at] if shared else mine, held.at[at], lat_send.at[0], sems.at[at], to
            )
            for mine, held, sems in ((latent, lat, lat_sem), (rope, rope_all, rope_sem))
        ]

    def send(name):
        m = by_name[name]
        if m.kind == "latent":
            for copy in latent_copies(name):
                copy.start()
            return
        sent = block(m, True)
        remote(
            sent, sent, w_send.at[SEND_KINDS.index(m.kind)], w_recv.at[number[m.group]],
            device(m.move["x"], m.move["y"], m.move["z"]),
        ).start()

    def lat_wait(at):
        await_bytes(lat.at[at], lat_sem.at[at])
        await_bytes(rope_all.at[at], rope_sem.at[at])

    def take(group):
        if group == ("next",):
            lat_wait(core)
        elif group == ("mate",):
            lat_wait(3 - core)
        elif group == ("share",):
            lat_wait(1 - core)
        elif len(members[group]) == 1:
            await_bytes(block(members[group][0], False), w_recv.at[number[group]])
        else:
            count = sum(m.size for m in members[group]) // 4096
            await_bytes(tiles(count), w_recv.at[number[group]])

    def q_copy(xi):
        return remote(
            q_part(1 - core, xi), qbuf.at[core, xi], q_send.at[0], q_sem.at[core], (seq, mate)
        )

    def setup():
        lat_wait(2 + core)
        length_copy.wait()
        lane = lax.broadcasted_iota(jnp.int32, (1, lengths.shape[1]), 1)
        start_own = jnp.sum(jnp.where(lane < slot, len_buf[...], 0), axis=1, keepdims=True)
        start_last = jnp.sum(jnp.where(lane < slot - 1, len_buf[...], 0), axis=1, keepdims=True)
        first = slot * 2 * tok
        q_place = first + lax.broadcasted_iota(jnp.int32, (2 * tok, 1), 0)
        begun = jnp.where(q_place >= start_own, start_own, start_last)
        k_place = first - 2 * tok + lax.broadcasted_iota(jnp.int32, (2 * tok, keys), 1)
        bias[...] = jnp.where((k_place >= begun) & (k_place <= q_place), 0.0, -jnp.inf)
        for at in range(4):
            turned = rope_all[at].astype(jnp.float32)
            tail = jnp.concatenate([turned, jnp.zeros_like(turned)], axis=0).T
            rows = slice(at * tok, (at + 1) * tok)
            for kaug in (kaug0, kaug1):
                kaug[0, rows, NOPE:] = tail.astype(jnp.bfloat16)
            rope_odd[rows, :] = pltpu.roll(tail, ROPE, axis=1)
        for pbuf in (pbuf0, pbuf1):
            pbuf[:, :tok, 3 * tok:] = jnp.zeros((2, tok, tok), jnp.bfloat16)
        for t in range(2):
            await_bytes(qbuf.at[t], q_sem.at[t])

    scale = LOG2E / math.sqrt(QK)
    held = ((kaug0, vbuf0, sbuf0, pbuf0, inv0), (kaug1, vbuf1, sbuf1, pbuf1, inv1))

    codes = [s * nx + off % nx for s, off in turns]

    def where(k):
        if isinstance(k, int):
            code = codes[k]
        else:
            code = jnp.int32(codes[0])
            for i in range(1, len(codes)):
                code = jnp.where(k == i, codes[i], code)
        return code // nx, (x + code % nx) % nx

    def weights(s, j, xi):
        parts = [w[UNITS * s + j + i, xi].reshape(n_seq * 16, 128) for i in range(2)]
        return jnp.concatenate(parts, axis=1)

    def project_keys(k, parity):
        s, xi = where(k)
        kaug = held[parity][0]
        low = lax.broadcasted_iota(jnp.int32, (keys, NOPE), 1) < ROPE
        k = jnp.dot(lat[...].reshape(keys, rank), weights(s, 0, xi), preferred_element_type=jnp.float32)
        kaug[0, :, :NOPE] = k[:, :NOPE].astype(jnp.bfloat16)
        turned = pltpu.roll(k[:, NOPE:], ROPE, axis=1)
        kaug[1, :, :NOPE] = jnp.where(low, 0.0, turned).astype(jnp.bfloat16)
        kaug[1, :, NOPE:] = jnp.where(low, turned, rope_odd[...]).astype(jnp.bfloat16)

    def project_values(k, parity):
        s, xi = where(k)
        v = jnp.dot(lat[...].reshape(keys, rank), weights(s, 2, xi), preferred_element_type=jnp.float32)
        held[parity][1][...] = v.astype(jnp.bfloat16)

    def score(k, parity):
        s, xi = where(k)
        kaug, _, sbuf, _, _ = held[parity]
        for h in range(2):
            begin = pl.multiple_of(s * 2 * QK + h * NOPE, 128)
            q = qbuf[:, xi, :, pl.ds(begin, 2 * NOPE)].reshape(2 * tok, 2 * NOPE)
            sc = lax.dot_general(
                q, kaug[h], (((1,), (1,)), ((), ())), preferred_element_type=jnp.float32
            )
            for t in range(2):
                rows, span = slice(t * tok, (t + 1) * tok), (3 + t) * tok
                sbuf[h, rows, :span] = sc[rows, :span] * scale + bias[rows, :span]

    def soften(parity):
        _, _, sbuf, pbuf, inv = held[parity]
        for t in range(2):
            span = (3 + t) * tok
            for h in range(2):
                for r in range(0, tok, CHUNK):
                    rows = slice(t * tok + r, t * tok + r + CHUNK)
                    sc = sbuf[h, rows, :span]
                    expo = jnp.exp2(sc - jnp.max(sc, axis=1, keepdims=True))
                    total = jnp.sum(expo, axis=1, keepdims=True)
                    inv[h, rows, :] = jnp.broadcast_to(1.0 / total, (CHUNK, VDIM))
                    pbuf[h, rows, :span] = expo.astype(jnp.bfloat16)

    def mix(k, parity):
        s, xi = where(k)
        _, vbuf, _, pbuf, inv = held[parity]
        for h in range(2):
            cols = slice(h * VDIM, (h + 1) * VDIM)
            mixed = jnp.dot(pbuf[h], vbuf[:, cols], preferred_element_type=jnp.float32)
            mixed = (mixed * inv[h]).astype(jnp.bfloat16)
            low, high = mixed[:tok], mixed[tok:]
            at = pl.multiple_of((2 * xi + core) * cw + s * 2 * VDIM + h * VDIM, 128)
            out[:, pl.ds(at, VDIM)] = jnp.where(core == 0, low, high)
            obuf[s, xi, :, cols] = jnp.where(core == 0, high, low)

    def give(k):
        s, xi = where(k)
        at = pl.multiple_of((2 * xi + core) * cw + s * 2 * VDIM, 128)
        landed = out.at[:, pl.ds(at, 2 * VDIM)]
        remote(obuf.at[s, xi], landed, o_sem.at[0], o_sem.at[1], (seq, mate)).start()

    def act(kind, name):
        if kind == "send":
            send(name)
        else:
            take(name)

    steps = stages * nx
    between, current = {}, "setup"
    for kind, name in [("piece", "setup")] + order:
        if kind != "piece":
            between[current].append((kind, name))
        elif name == "setup":
            current = "setup" if not between else "ready"
            between[current] = []
        else:
            current = name
            between[current] = []

    def events(name):
        for kind, what in between[name]:
            act(kind, what)

    def events_of(j, low, high, back):
        if not any(between["block", DEPTH + 2 * k + back] for k in range(low, high)):
            return
        if high - low == 1:
            events(("block", DEPTH + 2 * low + back))
            return
        middle = (low + high) // 2
        pl.when(j < middle)(functools.partial(events_of, j, low, middle, back))
        pl.when(j >= middle)(functools.partial(events_of, j, middle, high, back))

    def run(b, turn, first, last):
        if first <= 1 <= last:
            score(b - 1, (turn - 1) % 2)
        if first <= 2 <= last:
            soften(turn % 2)
        if first <= 0 <= last:
            project_keys(b, turn % 2)
        if first <= 2 <= last:
            project_values(b - 2, turn % 2)
        if first <= 3 <= last:
            mix(b - 3, (turn - 3) % 2)
            give(b - 3)

    events("setup")
    for xi in range(nx):
        q_copy(xi).start()
    setup()
    events("ready")
    for b in range(DEPTH):
        run(b, b, 0, b)
        events(("block", b))
    pairs = (steps - DEPTH) // 2

    def pair(j, carry):
        for back in range(2):
            run(DEPTH + 2 * j + back, DEPTH + back, 0, DEPTH)
            events_of(j, 0, pairs, back)
        return carry

    lax.fori_loop(0, pairs, pair, 0)
    for b in range(DEPTH + 2 * pairs, steps + DEPTH):
        run(b, b, max(0, b - steps + 1), DEPTH)
        events(("block", b))

    for i, kind in enumerate(SEND_KINDS):
        await_bytes(tiles(sent_tiles[kind]), w_send.at[i])
    await_bytes(tiles(3 * tok * (rank + ROPE) * 2 // 4096), lat_send.at[0])
    await_bytes(qbuf.at[core], q_send.at[0])
    for i in range(2):
        await_bytes(obuf, o_sem.at[i])


def shards(queries, latent, rope_keys, key_weight, value_weight, doc_lengths):
    n_seq, n_head = lax.axis_size("seq"), lax.axis_size("head")
    nx = n_head // 2
    tok, rank = latent.shape
    stages = key_weight.shape[1] // (2 * NOPE)
    docs = doc_lengths.shape[0]
    count = len({m.group for m in weight_messages(nx, n_seq // NY)})
    dma = pltpu.SemaphoreType.DMA
    bf16 = jnp.bfloat16
    return pl.pallas_call(
        functools.partial(kernel, (n_seq, n_head, stages)),
        out_shape=jax.ShapeDtypeStruct((tok, n_head * stages * 2 * VDIM), bf16),
        in_specs=[pl.BlockSpec(memory_space=pltpu.HBM)] * 6,
        out_specs=pl.BlockSpec(memory_space=pltpu.VMEM),
        scratch_shapes=[
            pltpu.VMEM((UNITS * stages, nx, n_seq // NY, NY, key_weight.shape[0], 128), bf16),
            pltpu.VMEM((4, tok, rank), bf16),
            pltpu.VMEM((4, ROPE, tok), bf16),
            pltpu.VMEM((2, nx, tok, 2 * stages * QK), bf16),
            pltpu.VMEM((2, 4 * tok, 2 * NOPE), bf16),
            pltpu.VMEM((2, 4 * tok, 2 * NOPE), bf16),
            pltpu.VMEM((4 * tok, 2 * ROPE), jnp.float32),
            pltpu.VMEM((4 * tok, 2 * VDIM), bf16),
            pltpu.VMEM((4 * tok, 2 * VDIM), bf16),
            pltpu.VMEM((2, 2 * tok, 4 * tok), jnp.float32),
            pltpu.VMEM((2, 2 * tok, 4 * tok), jnp.float32),
            pltpu.VMEM((2, 2 * tok, 4 * tok), bf16),
            pltpu.VMEM((2, 2 * tok, 4 * tok), bf16),
            pltpu.VMEM((2, 2 * tok, VDIM), jnp.float32),
            pltpu.VMEM((2, 2 * tok, VDIM), jnp.float32),
            pltpu.VMEM((2 * tok, 4 * tok), jnp.float32),
            pltpu.VMEM((stages, nx, tok, 2 * VDIM), bf16),
            pltpu.VMEM((1, docs), jnp.int32),
            dma((1,)),
            dma((4,)),
            dma((4,)),
            dma((1,)),
            dma((1,)),
            dma((count,)),
            dma((len(SEND_KINDS),)),
            dma((2,)),
            dma((1,)),
            dma((2,)),
        ],
        compiler_params=pltpu.CompilerParams(
            collective_id=0, has_side_effects=True, vmem_limit_bytes=48 * 2**20
        ),
    )(*[
        pltpu.with_memory_space_constraint(a, pltpu.HBM)
        for a in (queries, latent, rope_keys.T, key_weight, value_weight, doc_lengths.reshape(1, docs))
    ])


def solution(mesh):
    placed = (
        P(("seq", "head"), None),
        P(("seq", "head"), None),
        P(("seq", "head"), None),
        P("seq", "head"),
        P("seq", "head"),
        P(),
    )
    return jax.shard_map(
        shards, mesh=mesh, in_specs=placed, out_specs=P(("seq", "head"), None), check_vma=False
    )
```

```python
import collections
import functools
import math

import jax
import jax.numpy as jnp
from jax import lax
from jax.experimental import pallas as pl
from jax.experimental.pallas import tpu as pltpu
from jax.sharding import PartitionSpec as P

NOPE = 128
ROPE = 64
VDIM = 128
QK = NOPE + ROPE
LOG2E = 1.4426950408889634
NY = 4

MESH = pl.DeviceIdType.MESH

Stage = collections.namedtuple(
    "Stage", ("last", "far", "near_way", "far_way", "upwards", "split_side", "split_z")
)
STAGES = (
    Stage('x', 4, 0, -1, 7, 1, 1),
    Stage('y', 0, 0, -1, 4, 1, 1),
    Stage('y', 4, 0, 1, 6, 1, 1),
    Stage('x', 0, 0, 1, 5, 1, 0),
)
RANKS = (
    dict(near=2, z=8, far=10, farz=22, over=9, side=4),
    dict(near=1, z=7, far=5, farz=0, over=11, side=12),
    dict(near=6, z=24, far=19, farz=17, over=15, side=23),
    dict(near=18, z=16, far=3, farz=21, over=20, side=13),
)
LATENT_RANK = 14
UNITS = 4
RATE = 46.6e3
LATENCY = 3.6
HOP = 0.8
D2D_RATE = 300e3
BACKLOG = 0.5
SEND_COST = 0.04
WAIT_COST = 0.02
BLOCK = 0.8
DRAIN = (0.6, 0.5, 0.35)
DEPTH = 3
OFFSETS = (0, -1, 1, 2)
CHUNK = 32


class Message:
    def __init__(self, name, group, kind, deps, link, size, priority, units=None, where=None, move=None, hops=1):
        self.name, self.group, self.kind, self.deps, self.link = name, group, kind, deps, link
        self.size, self.priority, self.units, self.where = size, priority, units, where
        self.move, self.hops = move, hops


def weight_messages(nx, nz):
    tile = 16 * 128 * 2
    half = nz // 2
    found = []

    def add(name, group, kind, deps, axis, step, units, where, blocks):
        move = {"x": 0, "z": 0, "y": 0}
        move[axis] = step
        link = axis + ("+" if step > 0 else "-")
        rank = RANKS[name[0]][name[1]]
        found.append(Message(
            name, group, kind, deps, link, blocks * units[1] * tile, rank, units, where, move, abs(step)
        ))

    for s, stage in enumerate(STAGES):
        last, minor = stage.last, "y" if stage.last == "x" else "x"
        every, far = (UNITS * s, UNITS), (UNITS * s, stage.far)
        over = (UNITS * s + stage.far, UNITS - stage.far)

        def at(minor_at, last_at, z_at):
            return {minor: minor_at, last: last_at, "z": z_at}

        near = {k: (s, "near", k) for k in (1, -1, 2)}
        one_by_one = stage.near_way or stage.split_side or stage.split_z
        for k, name in near.items():
            group = name if one_by_one else (s, "near")
            if k == 2 and stage.near_way:
                way = stage.near_way
                add(name, group, "near", [near[way]], minor, way, every, at(-way, 0, 0), 1)
            else:
                add(name, group, "near", [], minor, k, every, at(0, 0, 0), 1)
        near = list(near.values())

        def first(name, group, kind, split, axis, way):
            if not split:
                add(name, group, kind, near, axis, way, every, at(None, 0, 0), 4)
                return [name]
            for k in (0, 1, -1, 2):
                add((*name, k), group, kind, [(s, "near", k)] if k else [], axis, way, every, at(-k, 0, 0), 1)
            return [(*name, k) for k in (0, 1, -1, 2)]

        reach = {1: half - s % 2, -1: half - 1 + s % 2}
        came = {0: near}
        for way in (1, -1):
            for d in range(1, reach[way] + 1):
                name = (s, "z", way, d)
                if d == 1:
                    came[-way] = first(name, name, "z", stage.split_z, "z", way)
                else:
                    add(name, name, "z", came[way * (1 - d)], "z", way, every, at(None, 0, way * (1 - d)), 4)
                    came[-way * d] = [name]
        if stage.far:
            name, way = (s, "far"), stage.far_way
            if way:
                deps = [(s, "side", way, 0, k) for k in (0, 1, -1, 2)] if stage.split_side else [(s, "side", way, 0)]
                add(name, name, "far", deps, last, way, far, at(None, -way, 0), 4)
            else:
                add(name, name, "far", near, last, 2, far, at(None, 0, 0), 4)
            for way in (1, -1):
                for d in range(1, reach[way] + 1):
                    deps = [(s, "far")] if d == 1 else [(s, "farz", way, d - 1)]
                    name = (s, "farz", way, d)
                    add(name, name, "far", deps, "z", way, far, at(None, 2, way * (1 - d)), 4)
        opposite = -half if s % 2 == 0 else half
        for i, r in enumerate((*range(0, -half, -1), opposite, *range(half - 1, 0, -1))):
            via = 1 if i < stage.upwards else -1
            for way in (1, -1):
                name = (s, "side", way, r)
                relayed = way == via and stage.far < UNITS
                alone = relayed or (r == 0 and stage.far and stage.far_way == way)
                group = name if alone else (s, "side", way, "rest")
                if r == 0:
                    names = first(name, group, "side", stage.split_side, last, way)
                else:
                    add(name, group, "side", came[r], last, way, every, at(None, 0, r), 4)
                    names = [name]
                if relayed:
                    deps = names
            if stage.far < UNITS:
                add((s, "over", via, r), (s, "over", via), "over", deps, last, via, over, at(None, -via, r), 4)
    return found


def latent_messages(tok, rank):
    size = tok * (rank + ROPE) * 2
    return [
        Message(("next",), ("next",), "latent", [], "x+", 1.3 * size, LATENT_RANK, hops=2),
        Message(("mate",), ("mate",), "latent", [], "d2d", size, LATENT_RANK),
        Message(("share",), ("share",), "latent", [("next",)], "d2d", size, LATENT_RANK),
    ]


def step_needs(messages, s, off):
    groups = {m.group for m in messages if m.name[0] == s}
    if STAGES[s].last == "y":
        return groups
    if off == 0:
        return {g for g in groups if g[1] in ("near", "z")}
    if off in (-1, 1):
        return {g for g in groups if g[1] == "side" and g[2] == -off}
    return {g for g in groups if g[1] in ("over", "far", "farz")}


def make_plan(messages):
    needs = {(s, off): step_needs(messages, s, off) for s in range(len(STAGES)) for off in OFFSETS}
    steps, able_steps, drained, prepared = [], [], 0, False
    group_of = {m.name: m.group for m in messages}
    left = {}
    for m in messages:
        left[m.group] = left.get(m.group, 0) + 1
    order, free, flying, seen = [], {}, [], set()
    waiting = sorted(messages, key=lambda m: m.priority)
    now = 0.0
    while waiting or flying or drained < DEPTH:
        flying.sort(key=lambda f: f[:2])
        if flying and flying[0][0] <= now:
            group = flying.pop(0)[2]
            left[group] -= 1
            if left[group] == 0:
                seen.add(group)
                order.append(("wait", group))
                now += WAIT_COST
                for step in [step for step, needed in needs.items() if needed <= seen]:
                    able_steps.append(step)
                    del needs[step]
            continue
        ready = [m for m in waiting if all(group_of[d] in seen for d in m.deps)]
        able = [m for m in ready if free.get(m.link, 0.0) - now < BACKLOG]
        if able:
            m = able[0]
            waiting.remove(m)
            order.append(("send", m.name))
            now += SEND_COST
            rate = D2D_RATE if m.link == "d2d" else RATE
            begun = max(now, free.get(m.link, 0.0))
            free[m.link] = begun + m.size * max(1, m.hops) / rate
            flying.append((free[m.link] + LATENCY + HOP * (m.hops - 1), len(order), m.group))
            continue
        if not prepared:
            if {("next",), ("mate",), ("share",)} <= seen:
                order.append(("piece", "setup"))
                now += BLOCK
                prepared = True
                continue
        elif able_steps:
            order.append(("piece", ("block", len(steps))))
            steps.append(able_steps.pop(0))
            now += BLOCK
            continue
        elif not needs and drained < DEPTH:
            order.append(("piece", ("block", len(steps) + drained)))
            now += DRAIN[drained]
            drained += 1
            continue
        times = [f[0] for f in flying[:1]] + [free[m.link] - BACKLOG for m in ready]
        now = max(now, min(times)) + 1e-6
    return order, steps, now


SEND_KINDS = ("near", "z", "far", "side", "over")


def kernel(
    sizes, queries, latent, rope, key_weight, value_weight, lengths, out,
    w, lat, rope_all, qbuf, kaug0, kaug1, rope_odd, vbuf0, vbuf1, sbuf0, sbuf1, pbuf0, pbuf1,
    inv0, inv1, bias, obuf, len_buf,
    own_sem, lat_sem, rope_sem, len_sem, lat_send, w_recv, w_send, q_sem, q_send, o_sem,
):
    n_seq, n_head, stages = sizes
    nx, ny, nz = n_head // 2, NY, n_seq // NY
    tok, rank = latent.shape
    keys = 4 * tok
    seq, head = lax.axis_index("seq"), lax.axis_index("head")
    x, core = head // 2, head % 2
    z, y = seq // ny, seq % ny
    mate = 2 * x + 1 - core
    slot = seq * nx + x
    after, before = (slot + 1) % (n_seq * nx), (slot + n_seq * nx - 1) % (n_seq * nx)

    messages = weight_messages(nx, nz)
    every = messages + latent_messages(tok, rank)
    order, turns, _ = make_plan(every)
    by_name = {m.name: m for m in every}
    groups = list(dict.fromkeys(m.group for m in messages))
    number = {g: i for i, g in enumerate(groups)}
    members = {g: [m for m in messages if m.group == g] for g in groups}
    sent_tiles = {kind: sum(m.size for m in messages if m.kind == kind) // 4096 for kind in SEND_KINDS}

    def device(dx, dy, dz):
        return ((z + dz) % nz) * ny + (y + dy) % ny, ((x + dx) % nx) * 2 + core

    def chip(which):
        return which // nx, (which % nx) * 2 + core

    barrier = pltpu.get_barrier_semaphore()
    peers = [device(k, 0, 0) for k in range(1, nx)] + [device(0, k, 0) for k in range(1, ny)]
    peers += [device(0, 0, 1), device(0, 0, nz - 1), (seq, mate), chip(after), chip(before)]
    for peer in peers:
        pl.semaphore_signal(barrier, inc=1, device_id=peer, device_id_type=MESH)

    for s in range(stages):
        for kv, source in enumerate((key_weight, value_weight)):
            for j in range(2):
                pltpu.make_async_copy(
                    source.at[:, pl.ds((2 * s + j) * 128, 128)],
                    w.at[UNITS * s + 2 * kv + j, x, z, y], own_sem.at[0],
                ).start()
    pltpu.make_async_copy(latent, lat.at[2 + core], lat_sem.at[2 + core]).start()
    pltpu.make_async_copy(rope, rope_all.at[2 + core], rope_sem.at[2 + core]).start()
    length_copy = pltpu.make_async_copy(lengths, len_buf, len_sem.at[0])
    length_copy.start()
    qw, cw = 2 * stages * QK, 2 * stages * VDIM

    def q_part(to_core, xi):
        return queries.at[:, pl.ds(pl.multiple_of((2 * xi + to_core) * qw, 128), qw)]

    for xi in range(nx):
        pltpu.make_async_copy(q_part(core, xi), qbuf.at[core, xi], q_sem.at[core]).start()

    def tiles(count):
        a, b, c, d = w.shape[:4]
        for k in range(1, d + 1):
            for j in range(1, c + 1):
                for i in range(1, b + 1):
                    if count % (i * j * k) == 0 and count // (i * j * k) <= a:
                        return w.at[pl.ds(0, count // (i * j * k)), pl.ds(0, i), pl.ds(0, j), pl.ds(0, k)]
        raise ValueError(count)

    def await_bytes(ref, sem):
        pltpu.make_async_copy(ref, ref, sem).wait()

    await_bytes(w.at[:, x, z, y], own_sem.at[0])
    pl.semaphore_wait(barrier, len(peers))

    def place(at, here, n):
        return pl.ds(0, n) if at is None else (here + at % n) % n

    def block(m, sent):
        def shifted(a):
            at = m.where[a]
            return at if at is None or sent else at - m.move[a]

        return w.at[
            pl.ds(*m.units), place(shifted("x"), x, nx), place(shifted("z"), z, nz), place(shifted("y"), y, ny)
        ]

    def remote(src, dst, send_sem, recv_sem, to):
        return pltpu.make_async_remote_copy(
            src_ref=src, dst_ref=dst, send_sem=send_sem, recv_sem=recv_sem,
            device_id=to, device_id_type=MESH,
        )

    def latent_copies(name):
        at = 2 + core if name == ("mate",) else core
        to = chip(after) if name == ("next",) else (seq, mate)
        shared = name == ("share",)
        return [
            remote(
                held.at[at] if shared else mine, held.at[at], lat_send.at[0], sems.at[at], to
            )
            for mine, held, sems in ((latent, lat, lat_sem), (rope, rope_all, rope_sem))
        ]

    def send(name):
        m = by_name[name]
        if m.kind == "latent":
            for copy in latent_copies(name):
                copy.start()
            return
        sent = block(m, True)
        remote(
            sent, sent, w_send.at[SEND_KINDS.index(m.kind)], w_recv.at[number[m.group]],
            device(m.move["x"], m.move["y"], m.move["z"]),
        ).start()

    def lat_wait(at):
        await_bytes(lat.at[at], lat_sem.at[at])
        await_bytes(rope_all.at[at], rope_sem.at[at])

    def take(group):
        if group == ("next",):
            lat_wait(core)
        elif group == ("mate",):
            lat_wait(3 - core)
        elif group == ("share",):
            lat_wait(1 - core)
        elif len(members[group]) == 1:
            await_bytes(block(members[group][0], False), w_recv.at[number[group]])
        else:
            count = sum(m.size for m in members[group]) // 4096
            await_bytes(tiles(count), w_recv.at[number[group]])

    def q_copy(xi):
        return remote(
            q_part(1 - core, xi), qbuf.at[core, xi], q_send.at[0], q_sem.at[core], (seq, mate)
        )

    def setup():
        lat_wait(2 + core)
        length_copy.wait()
        lane = lax.broadcasted_iota(jnp.int32, (1, lengths.shape[1]), 1)
        start_own = jnp.sum(jnp.where(lane < slot, len_buf[...], 0), axis=1, keepdims=True)
        start_last = jnp.sum(jnp.where(lane < slot - 1, len_buf[...], 0), axis=1, keepdims=True)
        first = slot * 2 * tok
        q_place = first + lax.broadcasted_iota(jnp.int32, (2 * tok, 1), 0)
        begun = jnp.where(q_place >= start_own, start_own, start_last)
        k_place = first - 2 * tok + lax.broadcasted_iota(jnp.int32, (2 * tok, keys), 1)
        bias[...] = jnp.where((k_place >= begun) & (k_place <= q_place), 0.0, -jnp.inf)
        for at in range(4):
            turned = rope_all[at].astype(jnp.float32)
            tail = jnp.concatenate([turned, jnp.zeros_like(turned)], axis=0).T
            rows = slice(at * tok, (at + 1) * tok)
            for kaug in (kaug0, kaug1):
                kaug[0, rows, NOPE:] = tail.astype(jnp.bfloat16)
            rope_odd[rows, :] = pltpu.roll(tail, ROPE, axis=1)
        for pbuf in (pbuf0, pbuf1):
            pbuf[:, :tok, 3 * tok:] = jnp.zeros((2, tok, tok), jnp.bfloat16)
        for t in range(2):
            await_bytes(qbuf.at[t], q_sem.at[t])

    scale = LOG2E / math.sqrt(QK)
    held = ((kaug0, vbuf0, sbuf0, pbuf0, inv0), (kaug1, vbuf1, sbuf1, pbuf1, inv1))

    codes = [s * nx + off % nx for s, off in turns]

    def where(k):
        if isinstance(k, int):
            code = codes[k]
        else:
            code = jnp.int32(codes[0])
            for i in range(1, len(codes)):
                code = jnp.where(k == i, codes[i], code)
        return code // nx, (x + code % nx) % nx

    def weights(s, j, xi):
        parts = [w[UNITS * s + j + i, xi].reshape(n_seq * 16, 128) for i in range(2)]
        return jnp.concatenate(parts, axis=1)

    def project_keys(k, parity):
        s, xi = where(k)
        kaug = held[parity][0]
        low = lax.broadcasted_iota(jnp.int32, (keys, NOPE), 1) < ROPE
        k = jnp.dot(lat[...].reshape(keys, rank), weights(s, 0, xi), preferred_element_type=jnp.float32)
        kaug[0, :, :NOPE] = k[:, :NOPE].astype(jnp.bfloat16)
        turned = pltpu.roll(k[:, NOPE:], ROPE, axis=1)
        kaug[1, :, :NOPE] = jnp.where(low, 0.0, turned).astype(jnp.bfloat16)
        kaug[1, :, NOPE:] = jnp.where(low, turned, rope_odd[...]).astype(jnp.bfloat16)

    def project_values(k, parity):
        s, xi = where(k)
        v = jnp.dot(lat[...].reshape(keys, rank), weights(s, 2, xi), preferred_element_type=jnp.float32)
        held[parity][1][...] = v.astype(jnp.bfloat16)

    def score(k, parity):
        s, xi = where(k)
        kaug, _, sbuf, _, _ = held[parity]
        for h in range(2):
            begin = pl.multiple_of(s * 2 * QK + h * NOPE, 128)
            q = qbuf[:, xi, :, pl.ds(begin, 2 * NOPE)].reshape(2 * tok, 2 * NOPE)
            sc = lax.dot_general(
                q, kaug[h], (((1,), (1,)), ((), ())), preferred_element_type=jnp.float32
            )
            for t in range(2):
                rows, span = slice(t * tok, (t + 1) * tok), (3 + t) * tok
                sbuf[h, rows, :span] = sc[rows, :span] * scale + bias[rows, :span]

    def soften(parity):
        _, _, sbuf, pbuf, inv = held[parity]
        for t in range(2):
            span = (3 + t) * tok
            for h in range(2):
                for r in range(0, tok, CHUNK):
                    rows = slice(t * tok + r, t * tok + r + CHUNK)
                    sc = sbuf[h, rows, :span]
                    expo = jnp.exp2(sc - jnp.max(sc, axis=1, keepdims=True))
                    total = jnp.sum(expo, axis=1, keepdims=True)
                    inv[h, rows, :] = jnp.broadcast_to(1.0 / total, (CHUNK, VDIM))
                    pbuf[h, rows, :span] = expo.astype(jnp.bfloat16)

    def mix(k, parity):
        s, xi = where(k)
        _, vbuf, _, pbuf, inv = held[parity]
        for h in range(2):
            cols = slice(h * VDIM, (h + 1) * VDIM)
            mixed = jnp.dot(pbuf[h], vbuf[:, cols], preferred_element_type=jnp.float32)
            mixed = (mixed * inv[h]).astype(jnp.bfloat16)
            low, high = mixed[:tok], mixed[tok:]
            at = pl.multiple_of((2 * xi + core) * cw + s * 2 * VDIM + h * VDIM, 128)
            out[:, pl.ds(at, VDIM)] = jnp.where(core == 0, low, high)
            obuf[s, xi, :, cols] = jnp.where(core == 0, high, low)

    def give(k):
        s, xi = where(k)
        at = pl.multiple_of((2 * xi + core) * cw + s * 2 * VDIM, 128)
        landed = out.at[:, pl.ds(at, 2 * VDIM)]
        remote(obuf.at[s, xi], landed, o_sem.at[0], o_sem.at[1], (seq, mate)).start()

    def act(kind, name):
        if kind == "send":
            send(name)
        else:
            take(name)

    steps = stages * nx
    between, current = {}, "setup"
    for kind, name in [("piece", "setup")] + order:
        if kind != "piece":
            between[current].append((kind, name))
        elif name == "setup":
            current = "setup" if not between else "ready"
            between[current] = []
        else:
            current = name
            between[current] = []

    def events(name):
        for kind, what in between[name]:
            act(kind, what)

    def events_of(j, low, high, back):
        if not any(between["block", DEPTH + 2 * k + back] for k in range(low, high)):
            return
        if high - low == 1:
            events(("block", DEPTH + 2 * low + back))
            return
        middle = (low + high) // 2
        pl.when(j < middle)(functools.partial(events_of, j, low, middle, back))
        pl.when(j >= middle)(functools.partial(events_of, j, middle, high, back))

    def run(b, turn, first, last):
        if first <= 0 <= last:
            project_keys(b, turn % 2)
        if first <= 2 <= last:
            project_values(b - 2, turn % 2)
        if first <= 1 <= last:
            score(b - 1, (turn - 1) % 2)
        if first <= 2 <= last:
            soften(turn % 2)
        if first <= 3 <= last:
            mix(b - 3, (turn - 3) % 2)
            give(b - 3)

    events("setup")
    for xi in range(nx):
        q_copy(xi).start()
    setup()
    events("ready")
    for b in range(DEPTH):
        run(b, b, 0, b)
        events(("block", b))
    pairs = (steps - DEPTH) // 2

    def pair(j, carry):
        for back in range(2):
            run(DEPTH + 2 * j + back, DEPTH + back, 0, DEPTH)
            events_of(j, 0, pairs, back)
        return carry

    lax.fori_loop(0, pairs, pair, 0)
    for b in range(DEPTH + 2 * pairs, steps + DEPTH):
        run(b, b, max(0, b - steps + 1), DEPTH)
        events(("block", b))

    for i, kind in enumerate(SEND_KINDS):
        await_bytes(tiles(sent_tiles[kind]), w_send.at[i])
    await_bytes(tiles(3 * tok * (rank + ROPE) * 2 // 4096), lat_send.at[0])
    await_bytes(qbuf.at[core], q_send.at[0])
    for i in range(2):
        await_bytes(obuf, o_sem.at[i])


def shards(queries, latent, rope_keys, key_weight, value_weight, doc_lengths):
    n_seq, n_head = lax.axis_size("seq"), lax.axis_size("head")
    nx = n_head // 2
    tok, rank = latent.shape
    stages = key_weight.shape[1] // (2 * NOPE)
    docs = doc_lengths.shape[0]
    count = len({m.group for m in weight_messages(nx, n_seq // NY)})
    dma = pltpu.SemaphoreType.DMA
    bf16 = jnp.bfloat16
    return pl.pallas_call(
        functools.partial(kernel, (n_seq, n_head, stages)),
        out_shape=jax.ShapeDtypeStruct((tok, n_head * stages * 2 * VDIM), bf16),
        in_specs=[pl.BlockSpec(memory_space=pltpu.HBM)] * 6,
        out_specs=pl.BlockSpec(memory_space=pltpu.VMEM),
        scratch_shapes=[
            pltpu.VMEM((UNITS * stages, nx, n_seq // NY, NY, key_weight.shape[0], 128), bf16),
            pltpu.VMEM((4, tok, rank), bf16),
            pltpu.VMEM((4, ROPE, tok), bf16),
            pltpu.VMEM((2, nx, tok, 2 * stages * QK), bf16),
            pltpu.VMEM((2, 4 * tok, 2 * NOPE), bf16),
            pltpu.VMEM((2, 4 * tok, 2 * NOPE), bf16),
            pltpu.VMEM((4 * tok, 2 * ROPE), jnp.float32),
            pltpu.VMEM((4 * tok, 2 * VDIM), bf16),
            pltpu.VMEM((4 * tok, 2 * VDIM), bf16),
            pltpu.VMEM((2, 2 * tok, 4 * tok), jnp.float32),
            pltpu.VMEM((2, 2 * tok, 4 * tok), jnp.float32),
            pltpu.VMEM((2, 2 * tok, 4 * tok), bf16),
            pltpu.VMEM((2, 2 * tok, 4 * tok), bf16),
            pltpu.VMEM((2, 2 * tok, VDIM), jnp.float32),
            pltpu.VMEM((2, 2 * tok, VDIM), jnp.float32),
            pltpu.VMEM((2 * tok, 4 * tok), jnp.float32),
            pltpu.VMEM((stages, nx, tok, 2 * VDIM), bf16),
            pltpu.VMEM((1, docs), jnp.int32),
            dma((1,)),
            dma((4,)),
            dma((4,)),
            dma((1,)),
            dma((1,)),
            dma((count,)),
            dma((len(SEND_KINDS),)),
            dma((2,)),
            dma((1,)),
            dma((2,)),
        ],
        compiler_params=pltpu.CompilerParams(
            collective_id=0, has_side_effects=True, vmem_limit_bytes=48 * 2**20
        ),
    )(*[
        pltpu.with_memory_space_constraint(a, pltpu.HBM)
        for a in (queries, latent, rope_keys.T, key_weight, value_weight, doc_lengths.reshape(1, docs))
    ])


def solution(mesh):
    placed = (
        P(("seq", "head"), None),
        P(("seq", "head"), None),
        P(("seq", "head"), None),
        P("seq", "head"),
        P("seq", "head"),
        P(),
    )
    return jax.shard_map(
        shards, mesh=mesh, in_specs=placed, out_specs=P(("seq", "head"), None), check_vma=False
    )
```

```python
import collections
import functools
import math

import jax
import jax.numpy as jnp
from jax import lax
from jax.experimental import pallas as pl
from jax.experimental.pallas import tpu as pltpu
from jax.sharding import PartitionSpec as P

NOPE = 128
ROPE = 64
VDIM = 128
QK = NOPE + ROPE
LOG2E = 1.4426950408889634
NY = 4

MESH = pl.DeviceIdType.MESH

Stage = collections.namedtuple(
    "Stage", ("last", "far", "near_way", "far_way", "upwards", "split_side", "split_z")
)
STAGES = (
    Stage('x', 4, 0, -1, 7, 1, 1),
    Stage('y', 0, 0, -1, 4, 1, 1),
    Stage('y', 4, 0, 1, 6, 1, 1),
    Stage('x', 0, 0, 1, 5, 1, 0),
)
RANKS = (
    dict(near=2, z=8, far=10, farz=22, over=9, side=4),
    dict(near=1, z=7, far=5, farz=0, over=11, side=12),
    dict(near=6, z=24, far=19, farz=17, over=15, side=23),
    dict(near=18, z=16, far=3, farz=21, over=20, side=13),
)
LATENT_RANK = 14
UNITS = 4
RATE = 46.6e3
LATENCY = 3.6
HOP = 0.8
D2D_RATE = 300e3
BACKLOG = 0.5
SEND_COST = 0.04
WAIT_COST = 0.02
BLOCK = 0.8
DRAIN = (0.6, 0.5, 0.35)
DEPTH = 3
OFFSETS = (0, -1, 1, 2)
CHUNK = 32


class Message:
    def __init__(self, name, group, kind, deps, link, size, priority, units=None, where=None, move=None, hops=1):
        self.name, self.group, self.kind, self.deps, self.link = name, group, kind, deps, link
        self.size, self.priority, self.units, self.where = size, priority, units, where
        self.move, self.hops = move, hops


def weight_messages(nx, nz):
    tile = 16 * 128 * 2
    half = nz // 2
    found = []

    def add(name, group, kind, deps, axis, step, units, where, blocks):
        move = {"x": 0, "z": 0, "y": 0}
        move[axis] = step
        link = axis + ("+" if step > 0 else "-")
        rank = RANKS[name[0]][name[1]]
        found.append(Message(
            name, group, kind, deps, link, blocks * units[1] * tile, rank, units, where, move, abs(step)
        ))

    for s, stage in enumerate(STAGES):
        last, minor = stage.last, "y" if stage.last == "x" else "x"
        every, far = (UNITS * s, UNITS), (UNITS * s, stage.far)
        over = (UNITS * s + stage.far, UNITS - stage.far)

        def at(minor_at, last_at, z_at):
            return {minor: minor_at, last: last_at, "z": z_at}

        near = {k: (s, "near", k) for k in (1, -1, 2)}
        one_by_one = stage.near_way or stage.split_side or stage.split_z
        for k, name in near.items():
            group = name if one_by_one else (s, "near")
            if k == 2 and stage.near_way:
                way = stage.near_way
                add(name, group, "near", [near[way]], minor, way, every, at(-way, 0, 0), 1)
            else:
                add(name, group, "near", [], minor, k, every, at(0, 0, 0), 1)
        near = list(near.values())

        def first(name, group, kind, split, axis, way):
            if not split:
                add(name, group, kind, near, axis, way, every, at(None, 0, 0), 4)
                return [name]
            for k in (0, 1, -1, 2):
                add((*name, k), group, kind, [(s, "near", k)] if k else [], axis, way, every, at(-k, 0, 0), 1)
            return [(*name, k) for k in (0, 1, -1, 2)]

        reach = {1: half - s % 2, -1: half - 1 + s % 2}
        came = {0: near}
        for way in (1, -1):
            for d in range(1, reach[way] + 1):
                name = (s, "z", way, d)
                if d == 1:
                    came[-way] = first(name, name, "z", stage.split_z, "z", way)
                else:
                    add(name, name, "z", came[way * (1 - d)], "z", way, every, at(None, 0, way * (1 - d)), 4)
                    came[-way * d] = [name]
        if stage.far:
            name, way = (s, "far"), stage.far_way
            if way:
                deps = [(s, "side", way, 0, k) for k in (0, 1, -1, 2)] if stage.split_side else [(s, "side", way, 0)]
                add(name, name, "far", deps, last, way, far, at(None, -way, 0), 4)
            else:
                add(name, name, "far", near, last, 2, far, at(None, 0, 0), 4)
            for way in (1, -1):
                for d in range(1, reach[way] + 1):
                    deps = [(s, "far")] if d == 1 else [(s, "farz", way, d - 1)]
                    name = (s, "farz", way, d)
                    add(name, name, "far", deps, "z", way, far, at(None, 2, way * (1 - d)), 4)
        opposite = -half if s % 2 == 0 else half
        for i, r in enumerate((*range(0, -half, -1), opposite, *range(half - 1, 0, -1))):
            via = 1 if i < stage.upwards else -1
            for way in (1, -1):
                name = (s, "side", way, r)
                relayed = way == via and stage.far < UNITS
                alone = relayed or (r == 0 and stage.far and stage.far_way == way)
                group = name if alone else (s, "side", way, "rest")
                if r == 0:
                    names = first(name, group, "side", stage.split_side, last, way)
                else:
                    add(name, group, "side", came[r], last, way, every, at(None, 0, r), 4)
                    names = [name]
                if relayed:
                    deps = names
            if stage.far < UNITS:
                add((s, "over", via, r), (s, "over", via), "over", deps, last, via, over, at(None, -via, r), 4)
    return found


def latent_messages(tok, rank):
    size = tok * (rank + ROPE) * 2
    return [
        Message(("next",), ("next",), "latent", [], "x+", 1.3 * size, LATENT_RANK, hops=2),
        Message(("mate",), ("mate",), "latent", [], "d2d", size, LATENT_RANK),
        Message(("share",), ("share",), "latent", [("next",)], "d2d", size, LATENT_RANK),
    ]


def step_needs(messages, s, off):
    groups = {m.group for m in messages if m.name[0] == s}
    if STAGES[s].last == "y":
        return groups
    if off == 0:
        return {g for g in groups if g[1] in ("near", "z")}
    if off in (-1, 1):
        return {g for g in groups if g[1] == "side" and g[2] == -off}
    return {g for g in groups if g[1] in ("over", "far", "farz")}


def make_plan(messages):
    needs = {(s, off): step_needs(messages, s, off) for s in range(len(STAGES)) for off in OFFSETS}
    steps, able_steps, drained, prepared = [], [], 0, False
    group_of = {m.name: m.group for m in messages}
    left = {}
    for m in messages:
        left[m.group] = left.get(m.group, 0) + 1
    order, free, flying, seen = [], {}, [], set()
    waiting = sorted(messages, key=lambda m: m.priority)
    now = 0.0
    while waiting or flying or drained < DEPTH:
        flying.sort(key=lambda f: f[:2])
        if flying and flying[0][0] <= now:
            group = flying.pop(0)[2]
            left[group] -= 1
            if left[group] == 0:
                seen.add(group)
                order.append(("wait", group))
                now += WAIT_COST
                for step in [step for step, needed in needs.items() if needed <= seen]:
                    able_steps.append(step)
                    del needs[step]
            continue
        ready = [m for m in waiting if all(group_of[d] in seen for d in m.deps)]
        able = [m for m in ready if free.get(m.link, 0.0) - now < BACKLOG]
        if able:
            m = able[0]
            waiting.remove(m)
            order.append(("send", m.name))
            now += SEND_COST
            rate = D2D_RATE if m.link == "d2d" else RATE
            begun = max(now, free.get(m.link, 0.0))
            free[m.link] = begun + m.size * max(1, m.hops) / rate
            flying.append((free[m.link] + LATENCY + HOP * (m.hops - 1), len(order), m.group))
            continue
        if not prepared:
            if {("next",), ("mate",), ("share",)} <= seen:
                order.append(("piece", "setup"))
                now += BLOCK
                prepared = True
                continue
        elif able_steps:
            order.append(("piece", ("block", len(steps))))
            steps.append(able_steps.pop(0))
            now += BLOCK
            continue
        elif not needs and drained < DEPTH:
            order.append(("piece", ("block", len(steps) + drained)))
            now += DRAIN[drained]
            drained += 1
            continue
        times = [f[0] for f in flying[:1]] + [free[m.link] - BACKLOG for m in ready]
        now = max(now, min(times)) + 1e-6
    return order, steps, now


SEND_KINDS = ("near", "z", "far", "side", "over")


def kernel(
    sizes, queries, latent, rope, key_weight, value_weight, lengths, out,
    w, lat, rope_all, qbuf, kaug0, kaug1, rope_odd, vbuf0, vbuf1, sbuf0, sbuf1, pbuf0, pbuf1,
    inv0, inv1, bias, obuf, len_buf,
    own_sem, lat_sem, rope_sem, len_sem, lat_send, w_recv, w_send, q_sem, q_send, o_sem,
):
    n_seq, n_head, stages = sizes
    nx, ny, nz = n_head // 2, NY, n_seq // NY
    tok, rank = latent.shape
    keys = 4 * tok
    seq, head = lax.axis_index("seq"), lax.axis_index("head")
    x, core = head // 2, head % 2
    z, y = seq // ny, seq % ny
    mate = 2 * x + 1 - core
    slot = seq * nx + x
    after, before = (slot + 1) % (n_seq * nx), (slot + n_seq * nx - 1) % (n_seq * nx)

    messages = weight_messages(nx, nz)
    every = messages + latent_messages(tok, rank)
    order, turns, _ = make_plan(every)
    by_name = {m.name: m for m in every}
    groups = list(dict.fromkeys(m.group for m in messages))
    number = {g: i for i, g in enumerate(groups)}
    members = {g: [m for m in messages if m.group == g] for g in groups}
    sent_tiles = {kind: sum(m.size for m in messages if m.kind == kind) // 4096 for kind in SEND_KINDS}

    def device(dx, dy, dz):
        return ((z + dz) % nz) * ny + (y + dy) % ny, ((x + dx) % nx) * 2 + core

    def chip(which):
        return which // nx, (which % nx) * 2 + core

    barrier = pltpu.get_barrier_semaphore()
    peers = [device(k, 0, 0) for k in range(1, nx)] + [device(0, k, 0) for k in range(1, ny)]
    peers += [device(0, 0, 1), device(0, 0, nz - 1), (seq, mate), chip(after), chip(before)]
    for peer in peers:
        pl.semaphore_signal(barrier, inc=1, device_id=peer, device_id_type=MESH)

    for s in range(stages):
        for kv, source in enumerate((key_weight, value_weight)):
            for j in range(2):
                pltpu.make_async_copy(
                    source.at[:, pl.ds((2 * s + j) * 128, 128)],
                    w.at[UNITS * s + 2 * kv + j, x, z, y], own_sem.at[0],
                ).start()
    pltpu.make_async_copy(latent, lat.at[2 + core], lat_sem.at[2 + core]).start()
    pltpu.make_async_copy(rope, rope_all.at[2 + core], rope_sem.at[2 + core]).start()
    length_copy = pltpu.make_async_copy(lengths, len_buf, len_sem.at[0])
    length_copy.start()
    qw, cw = 2 * stages * QK, 2 * stages * VDIM

    def q_part(to_core, xi):
        return queries.at[:, pl.ds(pl.multiple_of((2 * xi + to_core) * qw, 128), qw)]

    for xi in range(nx):
        pltpu.make_async_copy(q_part(core, xi), qbuf.at[core, xi], q_sem.at[core]).start()

    def tiles(count):
        a, b, c, d = w.shape[:4]
        for k in range(1, d + 1):
            for j in range(1, c + 1):
                for i in range(1, b + 1):
                    if count % (i * j * k) == 0 and count // (i * j * k) <= a:
                        return w.at[pl.ds(0, count // (i * j * k)), pl.ds(0, i), pl.ds(0, j), pl.ds(0, k)]
        raise ValueError(count)

    def await_bytes(ref, sem):
        pltpu.make_async_copy(ref, ref, sem).wait()

    await_bytes(w.at[:, x, z, y], own_sem.at[0])
    pl.semaphore_wait(barrier, len(peers))

    def place(at, here, n):
        return pl.ds(0, n) if at is None else (here + at % n) % n

    def block(m, sent):
        def shifted(a):
            at = m.where[a]
            return at if at is None or sent else at - m.move[a]

        return w.at[
            pl.ds(*m.units), place(shifted("x"), x, nx), place(shifted("z"), z, nz), place(shifted("y"), y, ny)
        ]

    def remote(src, dst, send_sem, recv_sem, to):
        return pltpu.make_async_remote_copy(
            src_ref=src, dst_ref=dst, send_sem=send_sem, recv_sem=recv_sem,
            device_id=to, device_id_type=MESH,
        )

    def latent_copies(name):
        at = 2 + core if name == ("mate",) else core
        to = chip(after) if name == ("next",) else (seq, mate)
        shared = name == ("share",)
        return [
            remote(
                held.at[at] if shared else mine, held.at[at], lat_send.at[0], sems.at[at], to
            )
            for mine, held, sems in ((latent, lat, lat_sem), (rope, rope_all, rope_sem))
        ]

    def send(name):
        m = by_name[name]
        if m.kind == "latent":
            for copy in latent_copies(name):
                copy.start()
            return
        sent = block(m, True)
        remote(
            sent, sent, w_send.at[SEND_KINDS.index(m.kind)], w_recv.at[number[m.group]],
            device(m.move["x"], m.move["y"], m.move["z"]),
        ).start()

    def lat_wait(at):
        await_bytes(lat.at[at], lat_sem.at[at])
        await_bytes(rope_all.at[at], rope_sem.at[at])

    def take(group):
        if group == ("next",):
            lat_wait(core)
        elif group == ("mate",):
            lat_wait(3 - core)
        elif group == ("share",):
            lat_wait(1 - core)
        elif len(members[group]) == 1:
            await_bytes(block(members[group][0], False), w_recv.at[number[group]])
        else:
            count = sum(m.size for m in members[group]) // 4096
            await_bytes(tiles(count), w_recv.at[number[group]])

    def q_copy(xi):
        return remote(
            q_part(1 - core, xi), qbuf.at[core, xi], q_send.at[0], q_sem.at[core], (seq, mate)
        )

    def setup():
        lat_wait(2 + core)
        length_copy.wait()
        lane = lax.broadcasted_iota(jnp.int32, (1, lengths.shape[1]), 1)
        start_own = jnp.sum(jnp.where(lane < slot, len_buf[...], 0), axis=1, keepdims=True)
        start_last = jnp.sum(jnp.where(lane < slot - 1, len_buf[...], 0), axis=1, keepdims=True)
        first = slot * 2 * tok
        q_place = first + lax.broadcasted_iota(jnp.int32, (2 * tok, 1), 0)
        begun = jnp.where(q_place >= start_own, start_own, start_last)
        k_place = first - 2 * tok + lax.broadcasted_iota(jnp.int32, (2 * tok, keys), 1)
        bias[...] = jnp.where((k_place >= begun) & (k_place <= q_place), 0.0, -jnp.inf)
        for at in range(4):
            turned = rope_all[at].astype(jnp.float32)
            tail = jnp.concatenate([turned, jnp.zeros_like(turned)], axis=0).T
            rows = slice(at * tok, (at + 1) * tok)
            for kaug in (kaug0, kaug1):
                kaug[0, rows, NOPE:] = tail.astype(jnp.bfloat16)
            rope_odd[rows, :] = pltpu.roll(tail, ROPE, axis=1)
        for pbuf in (pbuf0, pbuf1):
            pbuf[:, :tok, 3 * tok:] = jnp.zeros((2, tok, tok), jnp.bfloat16)
        for t in range(2):
            await_bytes(qbuf.at[t], q_sem.at[t])

    scale = LOG2E / math.sqrt(QK)
    held = ((kaug0, vbuf0, sbuf0, pbuf0, inv0), (kaug1, vbuf1, sbuf1, pbuf1, inv1))

    codes = [s * nx + off % nx for s, off in turns]

    def where(k):
        if isinstance(k, int):
            code = codes[k]
        else:
            code = jnp.int32(codes[0])
            for i in range(1, len(codes)):
                code = jnp.where(k == i, codes[i], code)
        return code // nx, (x + code % nx) % nx

    def weights(s, j, xi):
        parts = [w[UNITS * s + j + i, xi].reshape(n_seq * 16, 128) for i in range(2)]
        return jnp.concatenate(parts, axis=1)

    def project_keys(k, parity):
        s, xi = where(k)
        kaug = held[parity][0]
        low = lax.broadcasted_iota(jnp.int32, (keys, NOPE), 1) < ROPE
        k = jnp.dot(lat[...].reshape(keys, rank), weights(s, 0, xi), preferred_element_type=jnp.float32)
        kaug[0, :, :NOPE] = k[:, :NOPE].astype(jnp.bfloat16)
        turned = pltpu.roll(k[:, NOPE:], ROPE, axis=1)
        kaug[1, :, :NOPE] = jnp.where(low, 0.0, turned).astype(jnp.bfloat16)
        kaug[1, :, NOPE:] = jnp.where(low, turned, rope_odd[...]).astype(jnp.bfloat16)

    def project_values(k, parity):
        s, xi = where(k)
        v = jnp.dot(lat[...].reshape(keys, rank), weights(s, 2, xi), preferred_element_type=jnp.float32)
        held[parity][1][...] = v.astype(jnp.bfloat16)

    def score(k, parity):
        s, xi = where(k)
        kaug, _, sbuf, _, _ = held[parity]
        for h in range(2):
            begin = pl.multiple_of(s * 2 * QK + h * NOPE, 128)
            q = qbuf[:, xi, :, pl.ds(begin, 2 * NOPE)].reshape(2 * tok, 2 * NOPE)
            sc = lax.dot_general(
                q, kaug[h], (((1,), (1,)), ((), ())), preferred_element_type=jnp.float32
            )
            for t in range(2):
                rows, span = slice(t * tok, (t + 1) * tok), (3 + t) * tok
                sbuf[h, rows, :span] = sc[rows, :span] * scale + bias[rows, :span]

    def soften(parity):
        _, _, sbuf, pbuf, inv = held[parity]
        for t in range(2):
            span = (3 + t) * tok
            for h in range(2):
                for r in range(0, tok, CHUNK):
                    rows = slice(t * tok + r, t * tok + r + CHUNK)
                    sc = sbuf[h, rows, :span]
                    expo = jnp.exp2(sc - jnp.max(sc, axis=1, keepdims=True))
                    total = jnp.sum(expo, axis=1, keepdims=True)
                    inv[h, rows, :] = jnp.broadcast_to(1.0 / total, (CHUNK, VDIM))
                    pbuf[h, rows, :span] = expo.astype(jnp.bfloat16)

    def mix(k, parity):
        s, xi = where(k)
        _, vbuf, _, pbuf, inv = held[parity]
        for h in range(2):
            cols = slice(h * VDIM, (h + 1) * VDIM)
            mixed = jnp.dot(pbuf[h], vbuf[:, cols], preferred_element_type=jnp.float32)
            mixed = (mixed * inv[h]).astype(jnp.bfloat16)
            low, high = mixed[:tok], mixed[tok:]
            at = pl.multiple_of((2 * xi + core) * cw + s * 2 * VDIM + h * VDIM, 128)
            out[:, pl.ds(at, VDIM)] = jnp.where(core == 0, low, high)
            obuf[s, xi, :, cols] = jnp.where(core == 0, high, low)

    def give(k):
        s, xi = where(k)
        at = pl.multiple_of((2 * xi + core) * cw + s * 2 * VDIM, 128)
        landed = out.at[:, pl.ds(at, 2 * VDIM)]
        remote(obuf.at[s, xi], landed, o_sem.at[0], o_sem.at[1], (seq, mate)).start()

    def act(kind, name):
        if kind == "send":
            send(name)
        else:
            take(name)

    steps = stages * nx
    between, current = {}, "setup"
    for kind, name in [("piece", "setup")] + order:
        if kind != "piece":
            between[current].append((kind, name))
        elif name == "setup":
            current = "setup" if not between else "ready"
            between[current] = []
        else:
            current = name
            between[current] = []

    def events(name):
        for kind, what in between[name]:
            act(kind, what)

    def events_of(j, low, high, back):
        if not any(between["block", DEPTH + 2 * k + back] for k in range(low, high)):
            return
        if high - low == 1:
            events(("block", DEPTH + 2 * low + back))
            return
        middle = (low + high) // 2
        pl.when(j < middle)(functools.partial(events_of, j, low, middle, back))
        pl.when(j >= middle)(functools.partial(events_of, j, middle, high, back))

    def run(b, turn, first, last):
        if first <= 0 <= last:
            project_keys(b, turn % 2)
        if first <= 2 <= last:
            project_values(b - 2, turn % 2)
        if first <= 1 <= last:
            score(b - 1, (turn - 1) % 2)
        if first <= 2 <= last:
            soften(turn % 2)
        if first <= 3 <= last:
            mix(b - 3, (turn - 3) % 2)
            give(b - 3)

    for xi in range(nx):
        q_copy(xi).start()
    events("setup")
    setup()
    events("ready")
    for b in range(DEPTH):
        run(b, b, 0, b)
        events(("block", b))
    pairs = (steps - DEPTH) // 2

    def pair(j, carry):
        for back in range(2):
            run(DEPTH + 2 * j + back, DEPTH + back, 0, DEPTH)
            events_of(j, 0, pairs, back)
        return carry

    lax.fori_loop(0, pairs, pair, 0)
    for b in range(DEPTH + 2 * pairs, steps + DEPTH):
        run(b, b, max(0, b - steps + 1), DEPTH)
        events(("block", b))

    for i, kind in enumerate(SEND_KINDS):
        await_bytes(tiles(sent_tiles[kind]), w_send.at[i])
    await_bytes(tiles(3 * tok * (rank + ROPE) * 2 // 4096), lat_send.at[0])
    await_bytes(qbuf.at[core], q_send.at[0])
    for i in range(2):
        await_bytes(obuf, o_sem.at[i])


def shards(queries, latent, rope_keys, key_weight, value_weight, doc_lengths):
    n_seq, n_head = lax.axis_size("seq"), lax.axis_size("head")
    nx = n_head // 2
    tok, rank = latent.shape
    stages = key_weight.shape[1] // (2 * NOPE)
    docs = doc_lengths.shape[0]
    count = len({m.group for m in weight_messages(nx, n_seq // NY)})
    dma = pltpu.SemaphoreType.DMA
    bf16 = jnp.bfloat16
    return pl.pallas_call(
        functools.partial(kernel, (n_seq, n_head, stages)),
        out_shape=jax.ShapeDtypeStruct((tok, n_head * stages * 2 * VDIM), bf16),
        in_specs=[pl.BlockSpec(memory_space=pltpu.HBM)] * 6,
        out_specs=pl.BlockSpec(memory_space=pltpu.VMEM),
        scratch_shapes=[
            pltpu.VMEM((UNITS * stages, nx, n_seq // NY, NY, key_weight.shape[0], 128), bf16),
            pltpu.VMEM((4, tok, rank), bf16),
            pltpu.VMEM((4, ROPE, tok), bf16),
            pltpu.VMEM((2, nx, tok, 2 * stages * QK), bf16),
            pltpu.VMEM((2, 4 * tok, 2 * NOPE), bf16),
            pltpu.VMEM((2, 4 * tok, 2 * NOPE), bf16),
            pltpu.VMEM((4 * tok, 2 * ROPE), jnp.float32),
            pltpu.VMEM((4 * tok, 2 * VDIM), bf16),
            pltpu.VMEM((4 * tok, 2 * VDIM), bf16),
            pltpu.VMEM((2, 2 * tok, 4 * tok), jnp.float32),
            pltpu.VMEM((2, 2 * tok, 4 * tok), jnp.float32),
            pltpu.VMEM((2, 2 * tok, 4 * tok), bf16),
            pltpu.VMEM((2, 2 * tok, 4 * tok), bf16),
            pltpu.VMEM((2, 2 * tok, VDIM), jnp.float32),
            pltpu.VMEM((2, 2 * tok, VDIM), jnp.float32),
            pltpu.VMEM((2 * tok, 4 * tok), jnp.float32),
            pltpu.VMEM((stages, nx, tok, 2 * VDIM), bf16),
            pltpu.VMEM((1, docs), jnp.int32),
            dma((1,)),
            dma((4,)),
            dma((4,)),
            dma((1,)),
            dma((1,)),
            dma((count,)),
            dma((len(SEND_KINDS),)),
            dma((2,)),
            dma((1,)),
            dma((2,)),
        ],
        compiler_params=pltpu.CompilerParams(
            collective_id=0, has_side_effects=True, vmem_limit_bytes=48 * 2**20
        ),
    )(*[
        pltpu.with_memory_space_constraint(a, pltpu.HBM)
        for a in (queries, latent, rope_keys.T, key_weight, value_weight, doc_lengths.reshape(1, docs))
    ])


def solution(mesh):
    placed = (
        P(("seq", "head"), None),
        P(("seq", "head"), None),
        P(("seq", "head"), None),
        P("seq", "head"),
        P("seq", "head"),
        P(),
    )
    return jax.shard_map(
        shards, mesh=mesh, in_specs=placed, out_specs=P(("seq", "head"), None), check_vma=False
    )
```
